32 devices in a mesh: gx: 4 (over x, core), gy: 4 (over z), gz: 2 (over y).
Axes of the slice: x: 2, y: 2, z: 4, core: 2. Of those that a mesh axis runs over, the one named last changes fastest.
Arguments:
- velocity: float32 [3, 32, 128, 512], P(None, 'gz', 'gy', 'gx'), may hold values from -14 to 14, as said below
- geometry: bfloat16 [6, 32, 128, 512], P(None, 'gz', 'gy', 'gx'), may hold values from -0.015 to 0.041, as said below
- mass_weights: bfloat16 [32, 128, 512], P('gz', 'gy', 'gx'), may hold values from 0.0099487305 to 0.099609375
Outputs:
- residual: float32 [3, 32, 128, 512], P(None, 'gz', 'gy', 'gx')
- kinetic: float32 [], replicated
- enstrophy: float32 [], replicated
The draws below stay inside these ranges and needn't reach their ends.
Inputs may be any that keep to these rules, and one draw needn't show every extreme that they name: `velocity`: coincident points of neighbouring elements hold equal values, and points on the outer boundary of the grid hold zero. `geometry`: at every point the matrix [[g0, g3, g4], [g3, g1, g5], [g4, g5, g2]] is positive definite.
All inputs are finite; a program needn't handle non-finite values.
Results may differ from the reference program's by a relative error of at most 0.0003.
Values sent between devices are 32-bit elements; how exact they have to be, the bound alone decides.
A program may use at most 128 MiB of HBM per device.

```python
import math
import jax
import jax.numpy as jnp
import numpy as np
from jax import lax

ORDER = 7
POINTS = 8
GX = 512
GY = 128
GZ = 32


def join_faces(source, which_dim):
    position = lax.broadcasted_iota(jnp.int32, source.shape, which_dim)
    prev_val = jnp.roll(source, 1, which_dim)
    return jnp.where((position % (ORDER + 1) == 0) & (position > 0), prev_val, source)


def ramp_along(extent, which_dim):
    position = lax.broadcasted_iota(jnp.int32, extent, which_dim).astype(jnp.float32)
    return 0.5 + position / (extent[which_dim] - 1)


def draw_velocity(key, part):
    extent = (GZ, GY, GX)
    ramp_total = ramp_along(extent, 0) * ramp_along(extent, 1) * ramp_along(extent, 2)

    def one_component(comp_id):
        subkey = jax.random.fold_in(key, comp_id)
        noise = jnp.clip(jax.random.normal(subkey, extent, jnp.float32), -4.0, 4.0)
        field_now = noise * ramp_total
        field_now = join_faces(join_faces(join_faces(field_now, 2), 1), 0)
        inside = jnp.ones(extent, dtype=bool)
        for which_dim in range(3):
            position = lax.broadcasted_iota(jnp.int32, extent, which_dim)
            inside = inside & (position > 0) & (position < extent[which_dim] - 1)
        return jnp.where(inside, field_now, 0.0)
    return lax.map(one_component, jnp.arange(3)).astype(jnp.float32)


def draw_geometry(key, part):
    extent = (GZ, GY, GX)
    keyset = jax.random.split(key, 6)
    bottom, upper_end, reach = (0.003, 0.03, 0.3)
    diagonal = []
    for slot_id in range(3):
        drawn = jax.random.uniform(keyset[slot_id], extent, jnp.float32, math.log(bottom), math.log(upper_end))
        diagonal.append(jnp.exp(drawn))
    pairs_list = ((0, 1), (0, 2), (1, 2))
    offdiag = []
    for slot_id in range(3):
        first_id, second_id = pairs_list[slot_id]
        factor = jax.random.uniform(keyset[3 + slot_id], extent, jnp.float32, -reach, reach)
        offdiag.append(factor * jnp.sqrt(diagonal[first_id] * diagonal[second_id]))
    return jnp.stack(diagonal + offdiag, 0).astype(jnp.bfloat16)


def level_of(rng, shape, cuts, low, largest):
    level = 1.0
    for dim, shards_of in cuts:
        draws = jax.random.uniform(jax.random.fold_in(jax.random.fold_in(rng, 6), dim), (shards_of,), jnp.float32, low / len(cuts), largest / len(cuts))
        level = level * jnp.repeat(jnp.exp(draws), shape[dim] // shards_of).reshape((-1,) + (1,) * (len(shape) - 1 - dim))
    return level


def setup_inputs(seed: int = 0) -> dict:
    key_list = jax.random.split(jax.random.key(seed), 4)
    return {
        "velocity": draw_velocity(jax.random.fold_in(key_list[3], 71), 0),
        "geometry": draw_geometry(jax.random.fold_in(key_list[3], 71), 0),
        "mass_weights": jnp.clip(jnp.exp(math.log(0.099609375) - 2.3038113 * jax.random.uniform(key_list[2], (GZ, GY, GX), jnp.float32) ** level_of(key_list[2], (GZ, GY, GX), ((0, 2), (1, 4), (2, 4)), -0.2, 0.2)), 0.0099487305, 0.099609375).astype(jnp.bfloat16),
    }


def gll_derivative(poly_order):
    node_count = poly_order + 1
    abscissa = np.cos(np.pi * np.arange(node_count) / poly_order)
    legendre = np.zeros((node_count, node_count))
    for newton_step in range(60):
        legendre[:, 0] = 1.0
        legendre[:, 1] = abscissa
        for degree in range(2, node_count):
            legendre[:, degree] = ((2 * degree - 1) * abscissa * legendre[:, degree - 1] - (degree - 1) * legendre[:, degree - 2]) / degree
        abscissa = abscissa - (abscissa * legendre[:, poly_order] - legendre[:, poly_order - 1]) / (node_count * legendre[:, poly_order])
    abscissa = abscissa[::-1]
    end_values = legendre[::-1, poly_order]
    spacing = abscissa[:, None] - abscissa[None, :] + np.eye(node_count)
    deriv_table = end_values[:, None] / end_values[None, :] / spacing
    deriv_table = deriv_table * (1.0 - np.eye(node_count))
    deriv_table[0, 0] = -poly_order * node_count / 4.0
    deriv_table[poly_order, poly_order] = poly_order * node_count / 4.0
    return deriv_table.astype(np.float32)


def derive(source, matrix, which_dim):
    highest = lax.Precision.HIGHEST
    points = matrix.shape[0]
    extent = source.shape
    split_shape = extent[:which_dim] + (extent[which_dim] // points, points) + extent[which_dim + 1:]
    pieces = source.reshape(split_shape)
    if which_dim == 3:
        result = jnp.einsum('czyex,wx->czyew', pieces, matrix, precision=highest)
    elif which_dim == 2:
        result = jnp.einsum('czeyx,wy->czewx', pieces, matrix, precision=highest)
    else:
        result = jnp.einsum('cezyx,wz->cewyx', pieces, matrix, precision=highest)
    return result.reshape(extent)


def metric(geometry, slot_id):
    return geometry[slot_id].astype(jnp.float32)[None]


def apply_local(velocity, geometry, matrix):
    grad_r = derive(velocity, matrix, 3)
    grad_s = derive(velocity, matrix, 2)
    grad_t = derive(velocity, matrix, 1)
    flux_r = metric(geometry, 0) * grad_r + metric(geometry, 3) * grad_s + metric(geometry, 4) * grad_t
    flux_s = metric(geometry, 3) * grad_r + metric(geometry, 1) * grad_s + metric(geometry, 5) * grad_t
    flux_t = metric(geometry, 4) * grad_r + metric(geometry, 5) * grad_s + metric(geometry, 2) * grad_t
    enstrophy_part = jnp.sum(grad_r * flux_r + grad_s * flux_s + grad_t * flux_t)
    transposed = matrix.T
    applied = derive(flux_r, transposed, 3) + derive(flux_s, transposed, 2) + derive(flux_t, transposed, 1)
    return applied, enstrophy_part


def assemble_axis(source, which_dim):
    length = source.shape[which_dim]
    position = lax.broadcasted_iota(jnp.int32, source.shape, which_dim)
    next_val = jnp.roll(source, -1, which_dim)
    prev_val = jnp.roll(source, 1, which_dim)
    up_mask = (position % POINTS == POINTS - 1) & (position < length - 1)
    low_mask = (position % POINTS == 0) & (position > 0)
    return source + jnp.where(up_mask, next_val, 0.0) + jnp.where(low_mask, prev_val, 0.0)


def assemble_one(single_field):
    return assemble_axis(assemble_axis(assemble_axis(single_field, 2), 1), 0)


def reference(velocity, geometry, mass_weights):
    matrix = jnp.asarray(gll_derivative(ORDER), jnp.float32)
    mass_float = mass_weights.astype(jnp.float32)
    kinetic = 0.5 * jnp.sum(mass_float[None] * velocity * velocity)
    layers = velocity.shape[1] // POINTS

    def layer_step(layer_id, state_pair):
        applied, energy = state_pair
        offset = (layer_id * POINTS).astype(jnp.int32)
        block_vel = lax.dynamic_slice_in_dim(velocity, offset, POINTS, 1)
        block_geo = lax.dynamic_slice_in_dim(geometry, offset, POINTS, 1)
        part_field, part_energy = apply_local(block_vel, block_geo, matrix)
        applied = lax.dynamic_update_slice_in_dim(applied, part_field, offset, 1)
        return applied, energy + part_energy

    start_pair = (jnp.zeros(velocity.shape, jnp.float32), jnp.zeros((), jnp.float32))
    applied, enstrophy = lax.fori_loop(0, layers, layer_step, start_pair)
    stacked = jnp.concatenate([applied, mass_float[None]], 0)
    assembled = lax.map(assemble_one, stacked)
    extent = velocity.shape[1:]
    interior = jnp.ones(extent, dtype=bool)
    for which_dim in range(3):
        position = lax.broadcasted_iota(jnp.int32, extent, which_dim)
        interior = interior & (position > 0) & (position < extent[which_dim] - 1)
    rayleigh = enstrophy / (2.0 * kinetic)
    residual = jnp.where(interior[None], assembled[:3] - rayleigh * assembled[3][None] * velocity, 0.0)
    return residual, kinetic, enstrophy
```

```python
import functools
import itertools

import jax
import jax.numpy as jnp
import numpy as np
from jax import lax
from jax.experimental import pallas as pl
from jax.experimental.pallas import tpu as pltpu
from jax.sharding import PartitionSpec as P

ORDER = 7
PTS = ORDER + 1
MESH = pl.DeviceIdType.MESH
AXES = ("gx", "gy", "gz")
XOFF = [o for o in itertools.product((-1, 0, 1), repeat=3) if o[0] != 0]
YZOFF = [o for o in itertools.product((-1, 0, 1), repeat=3) if o[0] == 0 and o[1] != 0 and o[2] != 0]
YOFF = [(0, -1, 0), (0, 1, 0)]
FACES = YOFF + [(0, 0, -1), (0, 0, 1)]
OFFS = sorted(XOFF + YZOFF, key=lambda o: -sum(map(abs, o)))


def gll_derivative(poly_order):
    node_count = poly_order + 1
    abscissa = np.cos(np.pi * np.arange(node_count) / poly_order)
    legendre = np.zeros((node_count, node_count))
    for newton_step in range(60):
        legendre[:, 0] = 1.0
        legendre[:, 1] = abscissa
        for degree in range(2, node_count):
            legendre[:, degree] = (
                (2 * degree - 1) * abscissa * legendre[:, degree - 1]
                - (degree - 1) * legendre[:, degree - 2]
            ) / degree
        abscissa = abscissa - (abscissa * legendre[:, poly_order] - legendre[:, poly_order - 1]) / (
            node_count * legendre[:, poly_order]
        )
    abscissa = abscissa[::-1]
    end_values = legendre[::-1, poly_order]
    spacing = abscissa[:, None] - abscissa[None, :] + np.eye(node_count)
    deriv_table = end_values[:, None] / end_values[None, :] / spacing
    deriv_table = deriv_table * (1.0 - np.eye(node_count))
    deriv_table[0, 0] = -poly_order * node_count / 4.0
    deriv_table[poly_order, poly_order] = poly_order * node_count / 4.0
    return deriv_table.astype(np.float32)


def split_np(m):
    hi = m.astype(jnp.bfloat16)
    lo = (m - hi.astype(np.float32)).astype(jnp.bfloat16)
    return hi, lo


def tables(cols):
    d = gll_derivative(ORDER)
    eye = np.eye(PTS, dtype=np.float32)
    out = []
    for mat in (d, d.T):
        hi, lo = split_np(np.kron(np.eye(cols // PTS, dtype=np.float32), mat.T))
        zero = np.zeros_like(lo)
        out.append(np.block([[hi, lo], [hi, zero]]))
        hi, lo = split_np(np.concatenate([np.kron(eye, mat), np.kron(mat, eye)]))
        out.append(np.concatenate([hi, hi, lo, lo], axis=1))
    pick = np.zeros((2 * PTS, 2 * cols), np.float32)
    pick[0, [0, cols]] = 1.0
    pick[1, [cols - 1, 2 * cols - 1]] = 1.0
    out.append(pick.astype(jnp.bfloat16))
    put = np.zeros((16, 4 * cols), np.float32)
    for c in range(4):
        for base in (0, 8):
            put[base + c, c * cols + cols - 1] = 1.0
            put[base + 4 + c, c * cols] = 1.0
    out.append(put.astype(jnp.bfloat16))
    return [jnp.asarray(t) for t in out]


def split(x):
    hi = x.astype(jnp.bfloat16)
    lo = (x - hi.astype(jnp.float32)).astype(jnp.bfloat16)
    return hi, lo


def dot(a, b):
    return jnp.dot(a, b, preferred_element_type=jnp.float32)


def along_x(pair, table):
    cols = table.shape[1] // 2
    r = dot(jnp.concatenate(pair, axis=1), table)
    return r[:, :cols] + r[:, cols:]


def stacked(pairs):
    hi = jnp.concatenate([p[0] for p in pairs], axis=1)
    lo = jnp.concatenate([p[1] for p in pairs], axis=1)
    return jnp.concatenate([hi, lo, hi, lo], axis=0)


def kernel(
    sizes,
    v_hbm, g_hbm, m_hbm, dx_hbm, dyz_hbm, tx_hbm, tyz_hbm, pick_hbm, put_hbm,
    a_out, b_out, s_out,
    v, g, m, dx_ref, dyz_ref, tx_ref, tyz_ref, pick_ref, put_ref, flux, field, pack, yface, yzrow, rpack, ryface, rzface, ryz, part, parts, low, zface, keep, halo,
    in_sem, send_sem, recv_sem, ssend, srecv, lsend, lrecv, fsend, frecv,
):
    nx, ny, nz = sizes
    count = nx * ny * nz
    planes, rows, cols = v.shape[1:]
    layers = planes // PTS
    yel = rows // PTS
    ix, iy, iz = (lax.axis_index(a) for a in AXES)
    half = ny // 2
    n_low = half * nx * nz
    is_low = iy < half
    is_up = iy >= half

    def start(pairs, k):
        cs = [pltpu.make_async_copy(s, d, in_sem.at[k + i]) for i, (s, d) in enumerate(pairs)]
        for c in cs:
            c.start()
        return cs

    tabs = start([(dx_hbm, dx_ref), (dyz_hbm, dyz_ref)], 0)
    loads = []
    for e in range(layers):
        at = pl.ds(e * PTS, PTS)
        k = 2 + 3 * e
        loads.append(
            start([(v_hbm.at[:, at], v.at[:, at]), (m_hbm.at[at], m.at[at]), (g_hbm.at[:, at], g.at[:, at])], k)
        )
    late_tabs = start(
        [(tx_hbm, tx_ref), (tyz_hbm, tyz_ref), (pick_hbm, pick_ref), (put_hbm, put_ref)], 2 + 3 * layers
    )

    def rank(x, y, z):
        return (y * nx + x) * nz + z

    me = rank(ix, iy, iz)

    def for_targets(ys, act):
        if count > 64:
            def body(t):
                y, x, z = t // (nx * nz), lax.rem(t // nz, nx), lax.rem(t, nz)
                act((x, y, z), t != me)
            pl.loop(ys[0] * nx * nz, (ys[-1] + 1) * nx * nz)(body)
            return
        for y, x, z in itertools.product(ys, range(nx), range(nz)):
            act((x, y, z), rank(x, y, z) != me)

    lows, ups = range(half), range(half, ny)

    def dev(t):
        return dict(zip(AXES, t))

    barrier = pltpu.get_barrier_semaphore()

    def greet(t):
        pl.semaphore_signal(barrier, inc=1, device_id=dev(t), device_id_type=MESH)

    def greet_if(t, ok):
        pl.when(ok)(lambda: greet(t))

    def greet_low(t, ok):
        x, y, z = t
        near = (jnp.abs(ix - x) <= 1) & (jnp.abs(iz - z) <= 1) & (iy - y == 1)
        pl.when(near)(lambda: greet(t))

    for_targets(ups, greet_if)

    @pl.when(is_low)
    def _():
        for_targets(lows, greet_if)

    @pl.when(is_up)
    def _():
        for_targets(lows, greet_low)

    def cross(i, n):
        return 1 + jnp.where(i > 0, 1, 0) + jnp.where(i < n - 1, 1, 0)

    beyond = jnp.where(iy == half - 1, cross(ix, nx) * cross(iz, nz), 0)
    heard = jnp.where(is_low, n_low - 1 + beyond, count - 1)

    n_rows = PTS * rows
    four = (PTS, yel, PTS, cols)
    flat8 = (1, 1, PTS, cols)
    lane = lax.broadcasted_iota(jnp.int32, flat8, 3)
    k_at = lax.broadcasted_iota(jnp.int32, flat8, 2)

    def unit(mask):
        return jnp.where(mask, 1.0, 0.0).astype(jnp.float32)

    x_next = unit((lane % PTS == ORDER) & (lane < cols - 1))
    x_prev = unit((lane % PTS == 0) & (lane > 0))
    y_last = unit(k_at == ORDER)
    y_first = unit(k_at == 0)

    def assemble_xy(blocks):
        tiles = (PTS, PTS, cols)
        lane_next, lane_prev = x_next.reshape(1, PTS, cols), x_prev.reshape(1, PTS, cols)
        last, first = y_last.reshape(1, PTS, cols), y_first.reshape(1, PTS, cols)
        xs = []
        for x in blocks:
            up = pltpu.roll(x, cols - 1, 1).reshape(tiles)
            down = pltpu.roll(x, 1, 1).reshape(tiles)
            xs.append(x.reshape(tiles) + up * lane_next + down * lane_prev)
        out = []
        for y in range(yel):
            t = xs[y]
            if y < yel - 1:
                t = t + pltpu.roll(xs[y + 1], PTS - 1, 1) * last
            if y > 0:
                t = t + pltpu.roll(xs[y - 1], 1, 1) * first
            out.append(t)
        return out

    def put_field(c, e, blocks):
        for y, t in enumerate(assemble_xy(blocks)):
            field[c, pl.ds(e * PTS, PTS), y * PTS:(y + 1) * PTS, :] = t

    def finish_channel(c):
        for e in range(1, layers):
            low = field[c, e * PTS - 1]
            high = field[c, e * PTS]
            both = low + high
            field[c, e * PTS - 1] = both
            field[c, e * PTS] = both
        for e in range(layers):
            x = field[c, pl.ds(e * PTS, PTS)].reshape(n_rows, cols)
            r = lax.dot_general(
                pick_ref[...], jnp.concatenate(split(x), axis=1), (((1,), (1,)), ((), ())),
                preferred_element_type=jnp.float32,
            )
            for s in range(2):
                pack[s, pl.ds(c, 1), pl.ds(e * n_rows, n_rows)] = r[s:s + 1]
        for side, y in ((0, 0), (1, rows - 1)):
            face = field[c, :, y, :]
            yface[side, c] = face
            yzrow[side, 0, c] = face[0:1]
            yzrow[side, 1, c] = face[planes - 1:planes]
        zface[0, c] = field[c, 0]
        zface[1, c] = field[c, planes - 1]

    total_rows = planes * rows
    here = (ix, iy, iz)

    def there(off):
        ok = None
        for o, i, n in zip(off, here, sizes):
            if o:
                t = (i > 0) if o < 0 else (i < n - 1)
                ok = t if ok is None else ok & t
        return ok

    def side(o):
        return (o + 1) // 2

    def target(off):
        return {a: i + o for a, i, o in zip(AXES, here, off)}

    def part_of(dz):
        width = total_rows // layers // 2
        width = width if width % 128 == 0 else total_rows
        if dz == 0:
            return pl.ds(0, total_rows)
        return pl.ds(0 if dz < 0 else total_rows - width, width)

    def landing(off):
        if off[0]:
            return rpack.at[XOFF.index(off), :, part_of(-off[2])]
        return ryz.at[YZOFF.index(off)]

    def copy_to(off):
        opp = tuple(-o for o in off)
        if off[0]:
            src = pack.at[side(off[0]), :, part_of(off[2])]
        else:
            src = yzrow.at[side(off[1]), side(off[2])]
        return pltpu.make_async_remote_copy(
            src_ref=src, dst_ref=landing(opp), send_sem=send_sem.at[OFFS.index(off)],
            recv_sem=recv_sem.at[OFFS.index(opp)], device_id=target(off), device_id_type=MESH,
        )

    def face_copy(off, c):
        k, opp = FACES.index(off), FACES.index(tuple(-o for o in off))
        src, dst = (yface, ryface) if off[1] else (zface, rzface)
        return pltpu.make_async_remote_copy(
            src_ref=src.at[k % 2, c], dst_ref=dst.at[opp % 2, c], send_sem=fsend.at[k, c],
            recv_sem=frecv.at[opp, c], device_id=target(off), device_id_type=MESH,
        )

    def send_faces(c):
        for off in FACES[::-1]:
            @pl.when(there(off))
            def _(off=off):
                face_copy(off, c).start()

    inner_x = unit(((lane > 0) | (ix > 0)) & ((lane < cols - 1) | (ix < nx - 1))).reshape(1, PTS, cols)
    z3 = lax.broadcasted_iota(jnp.int32, (planes, 1, cols), 0)
    inner_z = unit(((z3 > 0) | (iz > 0)) & ((z3 < planes - 1) | (iz < nz - 1)))
    for y in range(yel):
        w = inner_x
        if y == 0:
            w = w * unit((k_at > 0) | (iy > 0)).reshape(1, PTS, cols)
        if y == yel - 1:
            w = w * unit((k_at < ORDER) | (iy < ny - 1)).reshape(1, PTS, cols)
        keep[:, y * PTS:(y + 1) * PTS, :] = w * inner_z
    for c in tabs:
        c.wait()
    zero = jnp.zeros((PTS, cols), jnp.float32)
    kin, ens = zero, zero
    n_blk = PTS * PTS
    for e in range(layers):
        for c in loads[e]:
            c.wait()
        at = pl.ds(e * PTS, PTS)
        mass = m[at].astype(jnp.float32)
        geo = [g[k, at].astype(jnp.float32) for k in range(6)]
        square = None
        for c in range(3):
            block = v[c, at]
            sq = block * block
            square = sq if square is None else square + sq
            blks = [block[:, y * PTS:(y + 1) * PTS, :].reshape(n_blk, cols) for y in range(yel)]
            pairs = [split(b) for b in blks]
            whole = tuple(jnp.concatenate([p[s] for p in pairs], axis=0) for s in range(2))
            gr_all = along_x(whole, dx_ref[...])
            for y0 in range(0, yel, 2):
                r = dot(dyz_ref[...], stacked(pairs[y0:y0 + 2]))
                for s in range(2):
                    y = y0 + s
                    tile = (PTS, PTS, cols)
                    gr = gr_all[y * n_blk:(y + 1) * n_blk].reshape(tile)
                    gs = r[:n_blk, s * cols:(s + 1) * cols].reshape(tile)
                    gt = r[n_blk:, s * cols:(s + 1) * cols].reshape(tile)
                    g0, g1, g2, g3, g4, g5 = (t[:, y * PTS:(y + 1) * PTS, :] for t in geo)
                    fr = g0 * gr + g3 * gs + g4 * gt
                    fs = g3 * gr + g1 * gs + g5 * gt
                    ft = g4 * gr + g5 * gs + g2 * gt
                    ens = ens + jnp.sum(gr * fr + gs * fs + gt * ft, axis=0)
                    flux[0, c, e, y] = fr
                    flux[1, c, e, y] = fs
                    flux[2, c, e, y] = ft
        kin = kin + jnp.sum((mass * square).reshape(-1, PTS, cols), axis=0)
    mine = jnp.concatenate(
        [jnp.sum(kin, 0, keepdims=True) * 0.5, jnp.sum(ens, 0, keepdims=True)], axis=0
    )
    part[...] = mine

    kind = jnp.where(is_up, 1, 0)

    def scalar_copy(to):
        return pltpu.make_async_remote_copy(
            src_ref=part, dst_ref=parts.at[me], send_sem=ssend, recv_sem=srecv.at[kind],
            device_id=to, device_id_type=MESH,
        )

    def tell(t, ok):
        pl.when(ok)(lambda: scalar_copy(dev(t)).start())

    def meet():
        pl.semaphore_wait(barrier, heard)
        for_targets(lows, tell)

        @pl.when(is_up)
        def _():
            for_targets(ups, tell)

    across = (nx - 1) // 2 - ix // 2 + (nz - 1 - iz)
    ahead = across + jnp.where(is_low, half - 1 - iy, ny - 1 - iy)
    turn = jnp.where((ix % 2 == 1) & (ix < nx - 1), 1, 0) + jnp.where(iz < nz - 1, 1, 0)
    ahead = jnp.where(iy == half - 1, jnp.maximum(ahead, 1 + turn), ahead)
    slot = jnp.where(ahead <= 1, -1, jnp.where(ahead == 2, 0, 2))

    @pl.when(slot < 0)
    def _():
        meet()
    parts[me] = mine

    for c in late_tabs:
        c.wait()
    for e in range(layers):
        x = m[pl.ds(e * PTS, PTS)].astype(jnp.float32)
        put_field(3, e, [x[:, y * PTS:(y + 1) * PTS, :].reshape(n_blk, cols) for y in range(yel)])
    finish_channel(3)

    @pl.loop(0, 3)
    def _(c):
        for e in range(layers):
            fr, fs, ft = ([split(flux[k, c, e, y].reshape(n_blk, cols)) for y in range(yel)] for k in range(3))
            whole = tuple(jnp.concatenate([p[s] for p in fr], axis=0) for s in range(2))
            x = along_x(whole, tx_ref[...])
            blocks = []
            for y0 in range(0, yel, 2):
                r = dot(tyz_ref[0:n_blk], stacked(fs[y0:y0 + 2])) + dot(tyz_ref[n_blk:], stacked(ft[y0:y0 + 2]))
                for s in range(2):
                    y = y0 + s
                    blocks.append(x[y * n_blk:(y + 1) * n_blk] + r[:, s * cols:(s + 1) * cols])
            put_field(c, e, blocks)
        finish_channel(c)
        pl.when(slot == c)(meet)

    for off in OFFS:
        @pl.when(there(off))
        def _(off=off):
            copy_to(off).start()

    for c in range(4):
        send_faces(c)

    def relay():
        return pltpu.make_async_remote_copy(
            src_ref=low, dst_ref=low, send_sem=lsend, recv_sem=lrecv,
            device_id={"gx": ix, "gy": iy + 1, "gz": iz}, device_id_type=MESH,
        )

    def wait_rows(n, sem):
        rest = parts.at[pl.ds(0, n)]
        pltpu.make_async_copy(rest, rest, sem).wait()

    def low_sum():
        wait_rows(n_low - 1, srecv.at[0])
        low[...] = jnp.sum(parts[0:n_low], axis=0)

    def low_wait():
        pltpu.make_async_copy(low, low, lrecv).wait()

    @pl.when(iy == half - 1)
    def _():
        low_sum()
        relay().start()

    @pl.when(is_up & (iy < ny - 1))
    def _():
        low_wait()
        relay().start()

    for off in OFFS:
        @pl.when(there(off))
        def _(off=off):
            dst = landing(off)
            pltpu.make_async_copy(dst, dst, recv_sem.at[OFFS.index(off)]).wait()

    for k, off in enumerate(FACES):
        @pl.when(there(off))
        def _(k=k, off=off):
            for c in range(4):
                dst = (ryface if off[1] else rzface).at[k % 2, c]
                pltpu.make_async_copy(dst, dst, frecv.at[k, c]).wait()

    pshape = (4, total_rows)
    place = lax.broadcasted_iota(jnp.int32, (1, total_rows), 1)
    for s, dx in ((0, 1), (1, -1)):
        acc = jnp.zeros(pshape, jnp.float32)
        for off in XOFF:
            if off[0] != dx:
                continue
            x = rpack[XOFF.index(off)]
            hit = place >= 0
            shift = 0
            if off[1]:
                hit = hit & (place % rows == (0 if off[1] < 0 else rows - 1))
                shift += off[1] * (rows - 1)
            if off[2]:
                hit = hit & (place // rows == (0 if off[2] < 0 else planes - 1))
                shift += off[2] * (planes - 1) * rows
            if shift:
                x = pltpu.roll(x, shift % total_rows, 1)
            acc = acc + jnp.where(jnp.broadcast_to(hit & there(off), pshape), x, 0.0)
        hi, lo = split(acc)
        halo[s * 4:s * 4 + 4, :] = hi.astype(jnp.float32)
        halo[8 + s * 4:12 + s * 4, :] = lo.astype(jnp.float32)

    z1 = lax.broadcasted_iota(jnp.int32, (planes, cols), 0)

    def add_yz(c):
        for dy, y in ((-1, 0), (1, rows - 1)):
            acc = jnp.where(there((0, dy, 0)), ryface[YOFF.index((0, dy, 0)), c], 0.0)
            for dz, z in ((-1, 0), (1, planes - 1)):
                off = (0, dy, dz)
                acc = acc + jnp.where((z1 == z) & there(off), ryz[YZOFF.index(off), c], 0.0)
            field[c, :, y, :] = field[c, :, y, :] + acc
        for k, (dz, z) in enumerate(((-1, 0), (1, planes - 1))):
            field[c, z] = field[c, z] + jnp.where(there((0, 0, dz)), rzface[k, c], 0.0)

    for c in range(4):
        add_yz(c)
    halos = halo[...].astype(jnp.bfloat16)
    for e in range(layers):
        at = pl.ds(e * PTS, PTS)
        x = lax.dot_general(
            halos[:, e * n_rows:(e + 1) * n_rows], put_ref[...], (((0,), (0,)), ((), ())),
            preferred_element_type=jnp.float32,
        )
        w = keep[at]
        mass = (field[3, at] + x[:, 3 * cols:].reshape(PTS, rows, cols)) * w
        for c in range(3):
            a_out[c, at] = (field[c, at] + x[:, c * cols:(c + 1) * cols].reshape(PTS, rows, cols)) * w
            b_out[c, at] = mass * v[c, at]

    for off in OFFS:
        @pl.when(there(off))
        def _(off=off):
            copy_to(off).wait_send()

    for off in FACES:
        @pl.when(there(off))
        def _(off=off):
            for c in range(4):
                face_copy(off, c).wait_send()

    n_up = count - n_low

    @pl.when(is_low)
    def _():
        wait_rows(n_low - 1, ssend)

    @pl.when(is_low & (iy < half - 1))
    def _():
        low_sum()

    @pl.when(is_up)
    def _():
        wait_rows(count - 1, ssend)

    @pl.when(iy == ny - 1)
    def _():
        low_wait()

    @pl.when((iy >= half - 1) & (iy < ny - 1))
    def _():
        relay().wait_send()

    @pl.when(is_low)
    def _():
        wait_rows(n_up, srecv.at[1])

    @pl.when(is_up)
    def _():
        wait_rows(n_up - 1, srecv.at[1])

    total = jnp.sum(parts[n_low:count], axis=0) + low[...]
    total = jnp.sum(total, axis=1, keepdims=True)
    s_out[...] = jnp.broadcast_to(total, (2, cols))


def finish(a_ref, b_ref, s_ref, r_hbm, k_hbm, e_hbm, r, k, e, sem):
    chunks = r.shape[0]
    kin = s_ref[0:1, :]
    ens = s_ref[1:2, :]
    rayleigh = ens / (2.0 * kin)
    k[...] = kin[:, 0:1]
    e[...] = ens[:, 0:1]
    outs = [
        pltpu.make_async_copy(k, k_hbm, sem.at[chunks]),
        pltpu.make_async_copy(e, e_hbm, sem.at[chunks + 1]),
    ]
    for c in range(chunks):
        r[c] = a_ref[c] - rayleigh[None] * b_ref[c]
        outs.append(pltpu.make_async_copy(r.at[c], r_hbm.at[c], sem.at[c]))
        outs[-1].start()
    outs[0].start()
    outs[1].start()
    for c in outs:
        c.wait()


def per_device(sizes, velocity, geometry, mass_weights):
    planes, rows, cols = mass_weights.shape
    f32 = jnp.float32
    count = sizes[0] * sizes[1] * sizes[2]
    vmem = pl.BlockSpec(memory_space=pltpu.VMEM)
    hbm = pl.BlockSpec(memory_space=pltpu.HBM)
    consts = tables(cols)
    layers = planes // PTS
    applied, weighted, scalars = pl.pallas_call(
        functools.partial(kernel, sizes),
        out_shape=(
            jax.ShapeDtypeStruct(velocity.shape, f32),
            jax.ShapeDtypeStruct(velocity.shape, f32),
            jax.ShapeDtypeStruct((2, cols), f32),
        ),
        in_specs=[hbm] * 9,
        out_specs=(vmem, vmem, vmem),
        scratch_shapes=[
            pltpu.VMEM(velocity.shape, f32),
            pltpu.VMEM(geometry.shape, geometry.dtype),
            pltpu.VMEM(mass_weights.shape, mass_weights.dtype),
            *[pltpu.VMEM(t.shape, t.dtype) for t in consts],
            pltpu.VMEM((3, 3, layers, rows // PTS, PTS, PTS, cols), f32),
            pltpu.VMEM((4, planes, rows, cols), f32),
            pltpu.VMEM((2, 4, planes * rows), f32),
            pltpu.VMEM((2, 4, planes, cols), f32),
            pltpu.VMEM((2, 2, 4, 1, cols), f32),
            pltpu.VMEM((len(XOFF), 4, planes * rows), f32),
            pltpu.VMEM((2, 4, planes, cols), f32),
            pltpu.VMEM((2, 4, rows, cols), f32),
            pltpu.VMEM((len(YZOFF), 4, 1, cols), f32),
            pltpu.VMEM((2, cols), f32),
            pltpu.VMEM((count, 2, cols), f32),
            pltpu.VMEM((2, cols), f32),
            pltpu.VMEM((2, 4, rows, cols), f32),
            pltpu.VMEM(mass_weights.shape, f32),
            pltpu.VMEM((16, planes * rows), f32),
            pltpu.SemaphoreType.DMA((6 + 3 * layers,)),
            pltpu.SemaphoreType.DMA((len(OFFS),)),
            pltpu.SemaphoreType.DMA((len(OFFS),)),
            pltpu.SemaphoreType.DMA,
            pltpu.SemaphoreType.DMA((2,)),
            pltpu.SemaphoreType.DMA,
            pltpu.SemaphoreType.DMA,
            pltpu.SemaphoreType.DMA((len(FACES), 4)),
            pltpu.SemaphoreType.DMA((len(FACES), 4)),
        ],
        compiler_params=pltpu.CompilerParams(
            collective_id=0, has_side_effects=True, vmem_limit_bytes=32 * 1024 * 1024
        ),
    )(*(pltpu.with_memory_space_constraint(t, pltpu.HBM) for t in (velocity, geometry, mass_weights, *consts)))
    one = jax.ShapeDtypeStruct((1, 1), f32)
    residual, kinetic, enstrophy = pl.pallas_call(
        finish,
        out_shape=(jax.ShapeDtypeStruct(velocity.shape, f32), one, one),
        in_specs=[vmem] * 3,
        out_specs=(hbm,) * 3,
        scratch_shapes=[
            pltpu.VMEM(velocity.shape, f32),
            pltpu.VMEM((1, 1), f32),
            pltpu.VMEM((1, 1), f32),
            pltpu.SemaphoreType.DMA((velocity.shape[0] + 2,)),
        ],
        compiler_params=pltpu.CompilerParams(vmem_limit_bytes=8 * 1024 * 1024),
    )(applied, weighted, scalars)
    return residual, kinetic[0, 0], enstrophy[0, 0]


def solution(mesh):
    sizes = tuple(mesh.shape[a] for a in AXES)
    in_specs = (P(None, "gz", "gy", "gx"), P(None, "gz", "gy", "gx"), P("gz", "gy", "gx"))
    out_specs = (P(None, "gz", "gy", "gx"), P(), P())
    return jax.shard_map(
        functools.partial(per_device, sizes),
        mesh=mesh, in_specs=in_specs, out_specs=out_specs, check_vma=False,
    )
```

```python
import functools
import itertools

import jax
import jax.numpy as jnp
import numpy as np
from jax import lax
from jax.experimental import pallas as pl
from jax.experimental.pallas import tpu as pltpu
from jax.sharding import PartitionSpec as P

ORDER = 7
PTS = ORDER + 1
MESH = pl.DeviceIdType.MESH
AXES = ("gx", "gy", "gz")
XOFF = [o for o in itertools.product((-1, 0, 1), repeat=3) if o[0] != 0]
YZOFF = [o for o in itertools.product((-1, 0, 1), repeat=3) if o[0] == 0 and o[1] != 0 and o[2] != 0]
YOFF = [(0, -1, 0), (0, 1, 0)]
FACES = YOFF + [(0, 0, -1), (0, 0, 1)]
OFFS = sorted(XOFF + YZOFF, key=lambda o: -sum(map(abs, o)))


def gll_derivative(poly_order):
    node_count = poly_order + 1
    abscissa = np.cos(np.pi * np.arange(node_count) / poly_order)
    legendre = np.zeros((node_count, node_count))
    for newton_step in range(60):
        legendre[:, 0] = 1.0
        legendre[:, 1] = abscissa
        for degree in range(2, node_count):
            legendre[:, degree] = (
                (2 * degree - 1) * abscissa * legendre[:, degree - 1]
                - (degree - 1) * legendre[:, degree - 2]
            ) / degree
        abscissa = abscissa - (abscissa * legendre[:, poly_order] - legendre[:, poly_order - 1]) / (
            node_count * legendre[:, poly_order]
        )
    abscissa = abscissa[::-1]
    end_values = legendre[::-1, poly_order]
    spacing = abscissa[:, None] - abscissa[None, :] + np.eye(node_count)
    deriv_table = end_values[:, None] / end_values[None, :] / spacing
    deriv_table = deriv_table * (1.0 - np.eye(node_count))
    deriv_table[0, 0] = -poly_order * node_count / 4.0
    deriv_table[poly_order, poly_order] = poly_order * node_count / 4.0
    return deriv_table.astype(np.float32)


def split_np(m):
    hi = m.astype(jnp.bfloat16)
    lo = (m - hi.astype(np.float32)).astype(jnp.bfloat16)
    return hi, lo


def tables(cols):
    d = gll_derivative(ORDER)
    eye = np.eye(PTS, dtype=np.float32)

    def lanes(mat):
        hi, lo = split_np(np.kron(np.eye(cols // PTS, dtype=np.float32), mat.T))
        return np.block([[hi, lo], [hi, np.zeros_like(lo)]])

    def paired(mat):
        hi, lo = split_np(mat)
        zero = np.zeros_like(hi)
        return np.concatenate([np.block([[t, t, zero, zero], [zero, zero, t, t]]) for t in (hi, lo)])

    hi, lo = split_np(np.concatenate([np.kron(eye, d), np.kron(d, eye)]))
    out = [lanes(d), np.concatenate([hi, hi, lo, lo], axis=1)]
    out.append(lanes(d.T))
    out.append(np.stack([paired(np.kron(eye, d.T)), paired(np.kron(d.T, eye))]))
    put = np.zeros((16, 4 * cols), np.float32)
    for c in range(4):
        for base in (0, 8):
            put[base + c, c * cols + cols - 1] = 1.0
            put[base + 4 + c, c * cols] = 1.0
    out.append(put.astype(jnp.bfloat16))
    return [jnp.asarray(t) for t in out]


def split(x):
    hi = x.astype(jnp.bfloat16)
    lo = (x - hi.astype(jnp.float32)).astype(jnp.bfloat16)
    return hi, lo


def dot(a, b):
    return jnp.dot(a, b, preferred_element_type=jnp.float32)


def along_x(pair, table):
    cols = table.shape[1] // 2
    r = dot(jnp.concatenate(pair, axis=1), table)
    return r[:, :cols] + r[:, cols:]


def tree(terms):
    while len(terms) > 1:
        odd = terms[len(terms) // 2 * 2:]
        terms = [a + b for a, b in zip(terms[::2], terms[1::2])] + odd
    return terms[0]


def quad(pairs):
    deep = [jnp.concatenate([*pairs[k], *pairs[k + 1]], axis=0) for k in (0, 2)]
    return jnp.concatenate(deep, axis=1)


def stacked(pairs):
    hi = jnp.concatenate([p[0] for p in pairs], axis=1)
    lo = jnp.concatenate([p[1] for p in pairs], axis=1)
    return jnp.concatenate([hi, lo, hi, lo], axis=0)


def kernel(
    sizes,
    v_hbm, g_hbm, m_hbm, dx_hbm, dyz_hbm, tx_hbm, tyz_hbm, put_hbm,
    a_out, b_out, s_out,
    v, g, m, dx_ref, dyz_ref, tx_ref, tyz_ref, put_ref, flux, field, ends, pack, yface, yzrow, rpack, ryface, rzface, ryz, part, parts, low, zface, keep, halo,
    in_sem, send_sem, recv_sem, ssend, srecv, lsend, lrecv, fsend, frecv,
):
    nx, ny, nz = sizes
    count = nx * ny * nz
    planes, rows, cols = v.shape[1:]
    layers = planes // PTS
    yel = rows // PTS
    ix, iy, iz = (lax.axis_index(a) for a in AXES)
    half = ny // 2
    n_low = half * nx * nz
    is_low = iy < half
    is_up = iy >= half

    def start(pairs, k):
        cs = [pltpu.make_async_copy(s, d, in_sem.at[k + i]) for i, (s, d) in enumerate(pairs)]
        for c in cs:
            c.start()
        return cs

    def load_layer(e):
        at = pl.ds(e * PTS, PTS)
        return start(
            [(v_hbm.at[:, at], v.at[:, at]), (g_hbm.at[:, at], g.at[:, at]), (m_hbm.at[at], m.at[at])], 2 + 3 * e
        )

    loads = [load_layer(0)]
    tabs = start([(dx_hbm, dx_ref), (dyz_hbm, dyz_ref)], 0)

    def rank(x, y, z):
        return (y * nx + x) * nz + z

    me = rank(ix, iy, iz)

    def for_targets(ys, act):
        if count > 64:
            def body(t):
                y, x, z = t // (nx * nz), lax.rem(t // nz, nx), lax.rem(t, nz)
                act((x, y, z), t != me)
            pl.loop(ys[0] * nx * nz, (ys[-1] + 1) * nx * nz)(body)
            return
        for y, x, z in itertools.product(ys, range(nx), range(nz)):
            act((x, y, z), rank(x, y, z) != me)

    lows, ups = range(half), range(half, ny)

    def dev(t):
        return dict(zip(AXES, t))

    barrier = pltpu.get_barrier_semaphore()

    def greet(t):
        pl.semaphore_signal(barrier, inc=1, device_id=dev(t), device_id_type=MESH)

    def greet_if(t, ok):
        pl.when(ok)(lambda: greet(t))

    def greet_low(t, ok):
        x, y, z = t
        near = (jnp.abs(ix - x) <= 1) & (jnp.abs(iz - z) <= 1) & (iy - y == 1)
        pl.when(near)(lambda: greet(t))

    for_targets(ups, greet_if)

    @pl.when(is_low)
    def _():
        for_targets(lows, greet_if)

    @pl.when(is_up)
    def _():
        for_targets(lows, greet_low)

    loads += [load_layer(e) for e in range(1, layers)]

    def cross(i, n):
        return 1 + jnp.where(i > 0, 1, 0) + jnp.where(i < n - 1, 1, 0)

    beyond = jnp.where(iy == half - 1, cross(ix, nx) * cross(iz, nz), 0)
    heard = jnp.where(is_low, n_low - 1 + beyond, count - 1)

    n_rows = PTS * rows
    four = (PTS, yel, PTS, cols)
    flat8 = (1, 1, PTS, cols)
    lane = lax.broadcasted_iota(jnp.int32, flat8, 3)
    k_at = lax.broadcasted_iota(jnp.int32, flat8, 2)

    def unit(mask):
        return jnp.where(mask, 1.0, 0.0).astype(jnp.float32)

    x_next = unit((lane % PTS == ORDER) & (lane < cols - 1))
    x_prev = unit((lane % PTS == 0) & (lane > 0))
    y_last = unit(k_at == ORDER)
    y_first = unit(k_at == 0)

    def assemble_xy(blocks):
        tiles = (PTS, PTS, cols)
        lane_next, lane_prev = x_next.reshape(1, PTS, cols), x_prev.reshape(1, PTS, cols)
        last, first = y_last.reshape(1, PTS, cols), y_first.reshape(1, PTS, cols)
        xs = []
        for x in blocks:
            up = pltpu.roll(x, cols - 1, 1).reshape(tiles)
            down = pltpu.roll(x, 1, 1).reshape(tiles)
            xs.append(x.reshape(tiles) + up * lane_next + down * lane_prev)
        out = []
        for y in range(yel):
            t = xs[y]
            if y < yel - 1:
                t = t + pltpu.roll(xs[y + 1], PTS - 1, 1) * last
            if y > 0:
                t = t + pltpu.roll(xs[y - 1], 1, 1) * first
            out.append(t)
        return out

    def put_field(c, e, blocks):
        for y, t in enumerate(assemble_xy(blocks)):
            field[c, pl.ds(e * PTS, PTS), y * PTS:(y + 1) * PTS, :] = t

    pair_of = lax.broadcasted_iota(jnp.int32, (rows, cols), 1) // 2

    def pack_sides():
        step = cols // rows
        for k in range(planes // step):
            t = ends[pl.ds(k * step, step)].reshape(cols, cols).T
            for c in range(4):
                for s in range(2):
                    r = 2 * c + 1 - s
                    pack[s, c:c + 1, k * cols:(k + 1) * cols] = t[r:r + 1]

    def finish_channel(c):
        for e in range(1, layers):
            low = field[c, e * PTS - 1]
            high = field[c, e * PTS]
            both = low + high
            field[c, e * PTS - 1] = both
            field[c, e * PTS] = both
        for k in range(planes):
            t = pltpu.roll(field[c, k], 2 * c + 1, 1)
            ends[k] = jnp.where(pair_of == c, t, 0.0 if c == 3 else ends[k])
        for side, y in ((0, 0), (1, rows - 1)):
            face = field[c, :, y, :]
            yface[side, c] = face
            yzrow[side, 0, c] = face[0:1]
            yzrow[side, 1, c] = face[planes - 1:planes]
        zface[0, c] = field[c, 0]
        zface[1, c] = field[c, planes - 1]

    total_rows = planes * rows
    here = (ix, iy, iz)

    def there(off):
        ok = None
        for o, i, n in zip(off, here, sizes):
            if o:
                t = (i > 0) if o < 0 else (i < n - 1)
                ok = t if ok is None else ok & t
        return ok

    def side(o):
        return (o + 1) // 2

    def target(off):
        return {a: i + o for a, i, o in zip(AXES, here, off)}

    def part_of(dz):
        width = total_rows // layers // 2
        width = width if width % 128 == 0 else total_rows
        if dz == 0:
            return pl.ds(0, total_rows)
        return pl.ds(0 if dz < 0 else total_rows - width, width)

    def landing(off):
        if off[0]:
            return rpack.at[XOFF.index(off), :, part_of(-off[2])]
        return ryz.at[YZOFF.index(off)]

    def copy_to(off):
        opp = tuple(-o for o in off)
        if off[0]:
            src = pack.at[side(off[0]), :, part_of(off[2])]
        else:
            src = yzrow.at[side(off[1]), side(off[2])]
        return pltpu.make_async_remote_copy(
            src_ref=src, dst_ref=landing(opp), send_sem=send_sem.at[OFFS.index(off)],
            recv_sem=recv_sem.at[OFFS.index(opp)], device_id=target(off), device_id_type=MESH,
        )

    def face_copy(off, c):
        k, opp = FACES.index(off), FACES.index(tuple(-o for o in off))
        src, dst = (yface, ryface) if off[1] else (zface, rzface)
        return pltpu.make_async_remote_copy(
            src_ref=src.at[k % 2, c], dst_ref=dst.at[opp % 2, c], send_sem=fsend.at[k, c],
            recv_sem=frecv.at[opp, c], device_id=target(off), device_id_type=MESH,
        )

    def send_faces(c):
        for off in FACES[::-1]:
            @pl.when(there(off))
            def _(off=off):
                face_copy(off, c).start()

    inner_x = unit(((lane > 0) | (ix > 0)) & ((lane < cols - 1) | (ix < nx - 1))).reshape(1, PTS, cols)
    z3 = lax.broadcasted_iota(jnp.int32, (planes, 1, cols), 0)
    inner_z = unit(((z3 > 0) | (iz > 0)) & ((z3 < planes - 1) | (iz < nz - 1)))
    for y in range(yel):
        w = inner_x
        if y == 0:
            w = w * unit((k_at > 0) | (iy > 0)).reshape(1, PTS, cols)
        if y == yel - 1:
            w = w * unit((k_at < ORDER) | (iy < ny - 1)).reshape(1, PTS, cols)
        keep[:, y * PTS:(y + 1) * PTS, :] = w * inner_z
    n_blk = PTS * PTS
    tile = (PTS, PTS, cols)
    kin, ens = [], []
    for e in range(layers):
        for c in loads[e] + (tabs if e == 0 else []):
            c.wait()
        if e == 0:
            late_tabs = start(
                [(tx_hbm, tx_ref), (tyz_hbm, tyz_ref), (put_hbm, put_ref)], 2 + 3 * layers
            )
        at = pl.ds(e * PTS, PTS)
        mass = m[at].astype(jnp.float32)
        geo = [g[k, at].astype(jnp.float32) for k in range(6)]
        square = None
        for c in range(3):
            block = v[c, at]
            square = block * block if square is None else square + block * block
            pairs = [split(block[:, y * PTS:(y + 1) * PTS, :].reshape(n_blk, cols)) for y in range(yel)]
            whole = tuple(jnp.concatenate([p[s] for p in pairs], axis=0) for s in range(2))
            gr_all = along_x(whole, dx_ref[...])
            for y0 in range(0, yel, 2):
                r = dot(dyz_ref[...], stacked(pairs[y0:y0 + 2]))
                for s in range(2):
                    y = y0 + s
                    gr = gr_all[y * n_blk:(y + 1) * n_blk].reshape(tile)
                    gs = r[:n_blk, s * cols:(s + 1) * cols].reshape(tile)
                    gt = r[n_blk:, s * cols:(s + 1) * cols].reshape(tile)
                    g0, g1, g2, g3, g4, g5 = (t[:, y * PTS:(y + 1) * PTS, :] for t in geo)
                    fr = g0 * gr + g3 * gs + g4 * gt
                    fs = g3 * gr + g1 * gs + g5 * gt
                    ft = g4 * gr + g5 * gs + g2 * gt
                    ens.append(jnp.sum(gr * fr + gs * fs + gt * ft, axis=0))
                    flux[0, c, e, y] = fr
                    flux[1, c, e, y] = fs
                    flux[2, c, e, y] = ft
        kin.append(jnp.sum((mass * square).reshape(-1, PTS, cols), axis=0))
    mine = jnp.concatenate(
        [jnp.sum(tree(kin), 0, keepdims=True) * 0.5, jnp.sum(tree(ens), 0, keepdims=True)], axis=0
    )
    part[...] = mine

    kind = jnp.where(is_up, 1, 0)

    def scalar_copy(to):
        return pltpu.make_async_remote_copy(
            src_ref=part, dst_ref=parts.at[me], send_sem=ssend, recv_sem=srecv.at[kind],
            device_id=to, device_id_type=MESH,
        )

    def tell(t, ok):
        pl.when(ok)(lambda: scalar_copy(dev(t)).start())

    def meet():
        pl.semaphore_wait(barrier, heard)
        for_targets(lows, tell)

        @pl.when(is_up)
        def _():
            for_targets(ups, tell)

    across = (nx - 1) // 2 - ix // 2 + (nz - 1 - iz)
    ahead = across + jnp.where(is_low, half - 1 - iy, ny - 1 - iy)
    turn = jnp.where((ix % 2 == 1) & (ix < nx - 1), 1, 0) + jnp.where(iz < nz - 1, 1, 0)
    ahead = jnp.where(iy == half - 1, jnp.maximum(ahead, 1 + turn), ahead)
    early = ahead <= 1

    @pl.when(early)
    def _():
        meet()
    parts[me] = mine

    for c in late_tabs:
        c.wait()
    for e in range(layers):
        x = m[pl.ds(e * PTS, PTS)].astype(jnp.float32)
        put_field(3, e, [x[:, y * PTS:(y + 1) * PTS, :].reshape(n_blk, cols) for y in range(yel)])
    finish_channel(3)

    for c in range(3):
        for e in range(layers):
            fr, fs, ft = ([split(flux[k, c, e, y].reshape(n_blk, cols)) for y in range(yel)] for k in range(3))
            whole = tuple(jnp.concatenate([p[s] for p in fr], axis=0) for s in range(2))
            x = along_x(whole, tx_ref[...])
            blocks = [x[y * n_blk:(y + 1) * n_blk] for y in range(yel)]
            for y0 in range(0, yel, 4):
                r = dot(tyz_ref[0], quad(fs[y0:y0 + 4])) + dot(tyz_ref[1], quad(ft[y0:y0 + 4]))
                r = r[:2 * n_blk] + r[2 * n_blk:]
                for s in range(4):
                    deep = (s % 2) * n_blk
                    blocks[y0 + s] += r[deep:deep + n_blk, (s // 2) * cols:(s // 2 + 1) * cols]
            put_field(c, e, blocks)
        finish_channel(c)

    pack_sides()
    pl.when(jnp.logical_not(early))(meet)

    for off in OFFS:
        @pl.when(there(off))
        def _(off=off):
            copy_to(off).start()

    for c in range(4):
        send_faces(c)

    odd = ix % 2 == 1

    def relays():
        return [
            pltpu.make_async_remote_copy(
                src_ref=low, dst_ref=low, send_sem=lsend.at[k], recv_sem=lrecv,
                device_id={"gx": ix - k, "gy": iy + 1, "gz": iz}, device_id_type=MESH,
            )
            for k in range(2)
        ]

    def relay_on():
        for c in relays():
            c.start()

    def wait_rows(n, sem):
        rest = parts.at[pl.ds(0, n)]
        pltpu.make_async_copy(rest, rest, sem).wait()

    def low_sum():
        wait_rows(n_low - 1, srecv.at[0])
        low[...] = jnp.sum(parts[0:n_low], axis=0)

    def low_wait():
        pltpu.make_async_copy(low, low, lrecv).wait()

    @pl.when((iy == half - 1) & odd)
    def _():
        low_sum()
        relay_on()

    @pl.when(is_up & (iy < ny - 1) & odd)
    def _():
        low_wait()
        relay_on()

    for off in OFFS:
        @pl.when(there(off))
        def _(off=off):
            dst = landing(off)
            pltpu.make_async_copy(dst, dst, recv_sem.at[OFFS.index(off)]).wait()

    for k, off in enumerate(FACES):
        @pl.when(there(off))
        def _(k=k, off=off):
            for c in range(4):
                dst = (ryface if off[1] else rzface).at[k % 2, c]
                pltpu.make_async_copy(dst, dst, frecv.at[k, c]).wait()

    pshape = (4, total_rows)
    place = lax.broadcasted_iota(jnp.int32, (1, total_rows), 1)
    for s, dx in ((0, 1), (1, -1)):
        acc = jnp.zeros(pshape, jnp.float32)
        for off in XOFF:
            if off[0] != dx:
                continue
            x = rpack[XOFF.index(off)]
            hit = place >= 0
            shift = 0
            if off[1]:
                hit = hit & (place % rows == (0 if off[1] < 0 else rows - 1))
                shift += off[1] * (rows - 1)
            if off[2]:
                hit = hit & (place // rows == (0 if off[2] < 0 else planes - 1))
                shift += off[2] * (planes - 1) * rows
            if shift:
                x = pltpu.roll(x, shift % total_rows, 1)
            acc = acc + jnp.where(jnp.broadcast_to(hit & there(off), pshape), x, 0.0)
        hi, lo = split(acc)
        halo[s * 4:s * 4 + 4, :] = hi.astype(jnp.float32)
        halo[8 + s * 4:12 + s * 4, :] = lo.astype(jnp.float32)

    z1 = lax.broadcasted_iota(jnp.int32, (planes, cols), 0)

    def add_yz(c):
        for dy, y in ((-1, 0), (1, rows - 1)):
            acc = jnp.where(there((0, dy, 0)), ryface[YOFF.index((0, dy, 0)), c], 0.0)
            for dz, z in ((-1, 0), (1, planes - 1)):
                off = (0, dy, dz)
                acc = acc + jnp.where((z1 == z) & there(off), ryz[YZOFF.index(off), c], 0.0)
            field[c, :, y, :] = field[c, :, y, :] + acc
        for k, (dz, z) in enumerate(((-1, 0), (1, planes - 1))):
            field[c, z] = field[c, z] + jnp.where(there((0, 0, dz)), rzface[k, c], 0.0)

    for c in range(4):
        add_yz(c)
    halos = halo[...].astype(jnp.bfloat16)
    for e in range(layers):
        at = pl.ds(e * PTS, PTS)
        x = lax.dot_general(
            halos[:, e * n_rows:(e + 1) * n_rows], put_ref[...], (((0,), (0,)), ((), ())),
            preferred_element_type=jnp.float32,
        )
        w = keep[at]
        mass = (field[3, at] + x[:, 3 * cols:].reshape(PTS, rows, cols)) * w
        for c in range(3):
            a_out[c, at] = (field[c, at] + x[:, c * cols:(c + 1) * cols].reshape(PTS, rows, cols)) * w
            b_out[c, at] = mass * v[c, at]

    for off in OFFS:
        @pl.when(there(off))
        def _(off=off):
            copy_to(off).wait_send()

    for off in FACES:
        @pl.when(there(off))
        def _(off=off):
            for c in range(4):
                face_copy(off, c).wait_send()

    n_up = count - n_low

    @pl.when(is_low)
    def _():
        wait_rows(n_low - 1, ssend)

    sends_on = (iy >= half - 1) & (iy < ny - 1) & odd
    later = jnp.logical_not(sends_on)

    @pl.when(is_low & later)
    def _():
        low_sum()

    @pl.when(is_up)
    def _():
        wait_rows(count - 1, ssend)

    @pl.when(is_up & later)
    def _():
        low_wait()

    @pl.when(sends_on)
    def _():
        for c in relays():
            c.wait_send()

    @pl.when(is_low)
    def _():
        wait_rows(n_up, srecv.at[1])

    @pl.when(is_up)
    def _():
        wait_rows(n_up - 1, srecv.at[1])

    total = jnp.sum(parts[n_low:count], axis=0) + low[...]
    total = jnp.sum(total, axis=1, keepdims=True)
    s_out[...] = jnp.broadcast_to(total, (2, cols))


def finish(a_ref, b_ref, s_ref, r_hbm, k_hbm, e_hbm, r, k, e, sem):
    chunks = r.shape[0]
    kin = s_ref[0:1, :]
    ens = s_ref[1:2, :]
    rayleigh = ens / (2.0 * kin)
    k[...] = kin[:, 0:1]
    e[...] = ens[:, 0:1]
    outs = [
        pltpu.make_async_copy(k, k_hbm, sem.at[chunks]),
        pltpu.make_async_copy(e, e_hbm, sem.at[chunks + 1]),
    ]
    for c in range(chunks):
        r[c] = a_ref[c] - rayleigh[None] * b_ref[c]
        outs.append(pltpu.make_async_copy(r.at[c], r_hbm.at[c], sem.at[c]))
        outs[-1].start()
    outs[0].start()
    outs[1].start()
    for c in outs:
        c.wait()


def per_device(sizes, velocity, geometry, mass_weights):
    planes, rows, cols = mass_weights.shape
    f32 = jnp.float32
    count = sizes[0] * sizes[1] * sizes[2]
    vmem = pl.BlockSpec(memory_space=pltpu.VMEM)
    hbm = pl.BlockSpec(memory_space=pltpu.HBM)
    consts = tables(cols)
    layers = planes // PTS
    applied, weighted, scalars = pl.pallas_call(
        functools.partial(kernel, sizes),
        out_shape=(
            jax.ShapeDtypeStruct(velocity.shape, f32),
            jax.ShapeDtypeStruct(velocity.shape, f32),
            jax.ShapeDtypeStruct((2, cols), f32),
        ),
        in_specs=[hbm] * 8,
        out_specs=(vmem, vmem, vmem),
        scratch_shapes=[
            pltpu.VMEM(velocity.shape, f32),
            pltpu.VMEM(geometry.shape, geometry.dtype),
            pltpu.VMEM(mass_weights.shape, mass_weights.dtype),
            *[pltpu.VMEM(t.shape, t.dtype) for t in consts],
            pltpu.VMEM((3, 3, layers, rows // PTS, PTS, PTS, cols), f32),
            pltpu.VMEM((4, planes, rows, cols), f32),
            pltpu.VMEM((planes, rows, cols), f32),
            pltpu.VMEM((2, 4, planes * rows), f32),
            pltpu.VMEM((2, 4, planes, cols), f32),
            pltpu.VMEM((2, 2, 4, 1, cols), f32),
            pltpu.VMEM((len(XOFF), 4, planes * rows), f32),
            pltpu.VMEM((2, 4, planes, cols), f32),
            pltpu.VMEM((2, 4, rows, cols), f32),
            pltpu.VMEM((len(YZOFF), 4, 1, cols), f32),
            pltpu.VMEM((2, cols), f32),
            pltpu.VMEM((count, 2, cols), f32),
            pltpu.VMEM((2, cols), f32),
            pltpu.VMEM((2, 4, rows, cols), f32),
            pltpu.VMEM(mass_weights.shape, f32),
            pltpu.VMEM((16, planes * rows), f32),
            pltpu.SemaphoreType.DMA((5 + 3 * layers,)),
            pltpu.SemaphoreType.DMA((len(OFFS),)),
            pltpu.SemaphoreType.DMA((len(OFFS),)),
            pltpu.SemaphoreType.DMA,
            pltpu.SemaphoreType.DMA((2,)),
            pltpu.SemaphoreType.DMA((2,)),
            pltpu.SemaphoreType.DMA,
            pltpu.SemaphoreType.DMA((len(FACES), 4)),
            pltpu.SemaphoreType.DMA((len(FACES), 4)),
        ],
        compiler_params=pltpu.CompilerParams(
            collective_id=0, has_side_effects=True, vmem_limit_bytes=32 * 1024 * 1024
        ),
    )(*(pltpu.with_memory_space_constraint(t, pltpu.HBM) for t in (velocity, geometry, mass_weights, *consts)))
    one = jax.ShapeDtypeStruct((1, 1), f32)
    residual, kinetic, enstrophy = pl.pallas_call(
        finish,
        out_shape=(jax.ShapeDtypeStruct(velocity.shape, f32), one, one),
        in_specs=[vmem] * 3,
        out_specs=(hbm,) * 3,
        scratch_shapes=[
            pltpu.VMEM(velocity.shape, f32),
            pltpu.VMEM((1, 1), f32),
            pltpu.VMEM((1, 1), f32),
            pltpu.SemaphoreType.DMA((velocity.shape[0] + 2,)),
        ],
        compiler_params=pltpu.CompilerParams(vmem_limit_bytes=8 * 1024 * 1024),
    )(applied, weighted, scalars)
    return residual, kinetic[0, 0], enstrophy[0, 0]


def solution(mesh):
    sizes = tuple(mesh.shape[a] for a in AXES)
    in_specs = (P(None, "gz", "gy", "gx"), P(None, "gz", "gy", "gx"), P("gz", "gy", "gx"))
    out_specs = (P(None, "gz", "gy", "gx"), P(), P())
    return jax.shard_map(
        functools.partial(per_device, sizes),
        mesh=mesh, in_specs=in_specs, out_specs=out_specs, check_vma=False,
    )
```

```python
import functools
import itertools
import math

import jax
import jax.numpy as jnp
import numpy as np
from jax import lax
from jax.experimental import pallas as pl
from jax.experimental.pallas import tpu as pltpu
from jax.sharding import PartitionSpec as P

ORDER = 7
PTS = ORDER + 1
UNIT = 4 * 128 * 4
MESH = pl.DeviceIdType.MESH
AXES = ("gx", "gy", "gz")
XOFF = [o for o in itertools.product((-1, 0, 1), repeat=3) if o[0] != 0]
YZOFF = [o for o in itertools.product((-1, 0, 1), repeat=3) if o[0] == 0 and o[1] != 0 and o[2] != 0]
YOFF = [(0, -1, 0), (0, 1, 0)]
FACES = YOFF + [(0, 0, -1), (0, 0, 1)]
OFFS = sorted(XOFF + YZOFF, key=lambda o: -sum(map(abs, o)))


def gll_derivative(poly_order):
    node_count = poly_order + 1
    abscissa = np.cos(np.pi * np.arange(node_count) / poly_order)
    legendre = np.zeros((node_count, node_count))
    for newton_step in range(60):
        legendre[:, 0] = 1.0
        legendre[:, 1] = abscissa
        for degree in range(2, node_count):
            legendre[:, degree] = (
                (2 * degree - 1) * abscissa * legendre[:, degree - 1]
                - (degree - 1) * legendre[:, degree - 2]
            ) / degree
        abscissa = abscissa - (abscissa * legendre[:, poly_order] - legendre[:, poly_order - 1]) / (
            node_count * legendre[:, poly_order]
        )
    abscissa = abscissa[::-1]
    end_values = legendre[::-1, poly_order]
    spacing = abscissa[:, None] - abscissa[None, :] + np.eye(node_count)
    deriv_table = end_values[:, None] / end_values[None, :] / spacing
    deriv_table = deriv_table * (1.0 - np.eye(node_count))
    deriv_table[0, 0] = -poly_order * node_count / 4.0
    deriv_table[poly_order, poly_order] = poly_order * node_count / 4.0
    return deriv_table.astype(np.float32)


def split_np(m):
    hi = m.astype(jnp.bfloat16)
    lo = (m - hi.astype(np.float32)).astype(jnp.bfloat16)
    return hi, lo


def tables(cols):
    d = gll_derivative(ORDER)
    eye = np.eye(PTS, dtype=np.float32)

    def lanes(mat):
        hi, lo = split_np(np.kron(np.eye(cols // PTS, dtype=np.float32), mat.T))
        return np.block([[hi, lo], [hi, np.zeros_like(lo)]])

    def paired(mat):
        hi, lo = split_np(mat)
        zero = np.zeros_like(hi)
        return np.concatenate([np.block([[t, t, zero, zero], [zero, zero, t, t]]) for t in (hi, lo)])

    hi, lo = split_np(np.concatenate([np.kron(eye, d), np.kron(d, eye)]))
    out = [lanes(d), np.concatenate([hi, hi, lo, lo], axis=1)]
    out.append(lanes(d.T))
    out.append(np.stack([paired(np.kron(eye, d.T)), paired(np.kron(d.T, eye))]))
    put = np.zeros((16, 4 * cols), np.float32)
    for c in range(4):
        for base in (0, 8):
            put[base + c, c * cols + cols - 1] = 1.0
            put[base + 4 + c, c * cols] = 1.0
    out.append(put.astype(jnp.bfloat16))
    return [jnp.asarray(t) for t in out]


def split(x):
    hi = x.astype(jnp.bfloat16)
    lo = (x - hi.astype(jnp.float32)).astype(jnp.bfloat16)
    return hi, lo


def dot(a, b):
    return jnp.dot(a, b, preferred_element_type=jnp.float32)


def along_x(pair, table):
    cols = table.shape[1] // 2
    r = dot(jnp.concatenate(pair, axis=1), table)
    return r[:, :cols] + r[:, cols:]


def tree(terms):
    while len(terms) > 1:
        odd = terms[len(terms) // 2 * 2:]
        terms = [a + b for a, b in zip(terms[::2], terms[1::2])] + odd
    return terms[0]


def quad(pairs):
    deep = [jnp.concatenate([*pairs[k], *pairs[k + 1]], axis=0) for k in (0, 2)]
    return jnp.concatenate(deep, axis=1)


def stacked(pairs):
    hi = jnp.concatenate([p[0] for p in pairs], axis=1)
    lo = jnp.concatenate([p[1] for p in pairs], axis=1)
    return jnp.concatenate([hi, lo, hi, lo], axis=0)


def kernel(
    sizes,
    v_hbm, g_hbm, m_hbm, dx_hbm, dyz_hbm, tx_hbm, tyz_hbm, put_hbm,
    a_out, b_out, s_out,
    v, g, m, dx_ref, dyz_ref, tx_ref, tyz_ref, put_ref, flux, field, ends, pack, yface, yzrow, rpack, ryface, rzface, ryz, part, parts, low, units, zface, keep, halo,
    in_sem, send_sem, recv_sem, ssend, srecv, lrecv,
):
    nx, ny, nz = sizes
    count = nx * ny * nz
    planes, rows, cols = v.shape[1:]
    layers = planes // PTS
    yel = rows // PTS
    ix, iy, iz = (lax.axis_index(a) for a in AXES)
    half = ny // 2
    n_low = half * nx * nz
    is_low = iy < half
    is_up = iy >= half

    def span(*refs):
        size = sum(math.prod(r.shape) * jnp.dtype(r.dtype).itemsize for r in refs)
        assert size % UNIT == 0
        return size // UNIT

    def await_units(n, sem):
        pltpu.make_async_copy(units.at[pl.ds(0, n)], units.at[pl.ds(0, n)], sem).wait()

    def start(pairs, k):
        for src, dst in pairs:
            pltpu.make_async_copy(src, dst, in_sem.at[k]).start()
        return span(*(dst for _, dst in pairs))

    def load_layer(e):
        at = pl.ds(e * PTS, PTS)
        return start(
            [(v_hbm.at[:, at], v.at[:, at]), (g_hbm.at[:, at], g.at[:, at]), (m_hbm.at[at], m.at[at])], e
        )

    loads = [load_layer(0)]
    loads[0] += start([(dx_hbm, dx_ref), (dyz_hbm, dyz_ref)], 0)

    def rank(x, y, z):
        return (y * nx + x) * nz + z

    me = rank(ix, iy, iz)

    def for_targets(ys, act):
        if count > 64:
            def body(t):
                y, x, z = t // (nx * nz), lax.rem(t // nz, nx), lax.rem(t, nz)
                act((x, y, z), t != me)
            pl.loop(ys[0] * nx * nz, (ys[-1] + 1) * nx * nz)(body)
            return
        for y, x, z in itertools.product(ys, range(nx), range(nz)):
            act((x, y, z), rank(x, y, z) != me)

    lows, ups = range(half), range(half, ny)

    def dev(t):
        return dict(zip(AXES, t))

    barrier = pltpu.get_barrier_semaphore()

    def greet(t):
        pl.semaphore_signal(barrier, inc=1, device_id=dev(t), device_id_type=MESH)

    def greet_if(t, ok):
        pl.when(ok)(lambda: greet(t))

    def greet_low(t, ok):
        x, y, z = t
        near = (jnp.abs(ix - x) <= 1) & (jnp.abs(iz - z) <= 1) & (iy - y == 1)
        pl.when(near)(lambda: greet(t))

    for_targets(ups, greet_if)

    @pl.when(is_low)
    def _():
        for_targets(lows, greet_if)

    @pl.when(is_up)
    def _():
        for_targets(lows, greet_low)

    loads += [load_layer(e) for e in range(1, layers)]

    def cross(i, n):
        return 1 + jnp.where(i > 0, 1, 0) + jnp.where(i < n - 1, 1, 0)

    beyond = jnp.where(iy == half - 1, cross(ix, nx) * cross(iz, nz), 0)
    heard = jnp.where(is_low, n_low - 1 + beyond, count - 1)

    n_rows = PTS * rows
    four = (PTS, yel, PTS, cols)
    flat8 = (1, 1, PTS, cols)
    lane = lax.broadcasted_iota(jnp.int32, flat8, 3)
    k_at = lax.broadcasted_iota(jnp.int32, flat8, 2)

    def unit(mask):
        return jnp.where(mask, 1.0, 0.0).astype(jnp.float32)

    x_next = unit((lane % PTS == ORDER) & (lane < cols - 1))
    x_prev = unit((lane % PTS == 0) & (lane > 0))
    y_last = unit(k_at == ORDER)
    y_first = unit(k_at == 0)

    def assemble_xy(blocks):
        tiles = (PTS, PTS, cols)
        lane_next, lane_prev = x_next.reshape(1, PTS, cols), x_prev.reshape(1, PTS, cols)
        last, first = y_last.reshape(1, PTS, cols), y_first.reshape(1, PTS, cols)
        xs = []
        for x in blocks:
            up = pltpu.roll(x, cols - 1, 1).reshape(tiles)
            down = pltpu.roll(x, 1, 1).reshape(tiles)
            xs.append(x.reshape(tiles) + up * lane_next + down * lane_prev)
        out = []
        for y in range(yel):
            t = xs[y]
            if y < yel - 1:
                t = t + pltpu.roll(xs[y + 1], PTS - 1, 1) * last
            if y > 0:
                t = t + pltpu.roll(xs[y - 1], 1, 1) * first
            out.append(t)
        return out

    def put_field(c, e, blocks):
        for y, t in enumerate(assemble_xy(blocks)):
            field[c, pl.ds(e * PTS, PTS), y * PTS:(y + 1) * PTS, :] = t

    pair_of = lax.broadcasted_iota(jnp.int32, (rows, cols), 1) // 2

    def pack_sides():
        step = cols // rows
        for k in range(planes // step):
            t = ends[pl.ds(k * step, step)].reshape(cols, cols).T
            for c in range(4):
                for s in range(2):
                    r = 2 * c + 1 - s
                    pack[s, c:c + 1, k * cols:(k + 1) * cols] = t[r:r + 1]

    def finish_channel(c):
        for e in range(1, layers):
            low = field[c, e * PTS - 1]
            high = field[c, e * PTS]
            both = low + high
            field[c, e * PTS - 1] = both
            field[c, e * PTS] = both
        for k in range(planes):
            t = pltpu.roll(field[c, k], 2 * c + 1, 1)
            ends[k] = jnp.where(pair_of == c, t, 0.0 if c == 3 else ends[k])
        for side, y in ((0, 0), (1, rows - 1)):
            face = field[c, :, y, :]
            yface[side, c] = face
            yzrow[side, 0, c] = face[0:1]
            yzrow[side, 1, c] = face[planes - 1:planes]
        zface[0, c] = field[c, 0]
        zface[1, c] = field[c, planes - 1]

    total_rows = planes * rows
    here = (ix, iy, iz)

    def there(off):
        ok = None
        for o, i, n in zip(off, here, sizes):
            if o:
                t = (i > 0) if o < 0 else (i < n - 1)
                ok = t if ok is None else ok & t
        return ok

    def side(o):
        return (o + 1) // 2

    def target(off):
        return {a: i + o for a, i, o in zip(AXES, here, off)}

    def part_of(dz):
        width = total_rows // layers // 2
        width = width if width % 128 == 0 else total_rows
        if dz == 0:
            return pl.ds(0, total_rows)
        return pl.ds(0 if dz < 0 else total_rows - width, width)

    def landing(off):
        if off[0]:
            return rpack.at[XOFF.index(off), :, part_of(-off[2])]
        return ryz.at[YZOFF.index(off)]

    def copy_to(off):
        opp = tuple(-o for o in off)
        if off[0]:
            src = pack.at[side(off[0]), :, part_of(off[2])]
        else:
            src = yzrow.at[side(off[1]), side(off[2])]
        return pltpu.make_async_remote_copy(
            src_ref=src, dst_ref=landing(opp), send_sem=send_sem, recv_sem=recv_sem,
            device_id=target(off), device_id_type=MESH,
        )

    def face_copy(off, c):
        k, opp = FACES.index(off), FACES.index(tuple(-o for o in off))
        src, dst = (yface, ryface) if off[1] else (zface, rzface)
        return pltpu.make_async_remote_copy(
            src_ref=src.at[k % 2, c], dst_ref=dst.at[opp % 2, c], send_sem=send_sem,
            recv_sem=recv_sem, device_id=target(off), device_id_type=MESH,
        )

    def send_faces(c):
        for off in FACES[::-1]:
            @pl.when(there(off))
            def _(off=off):
                face_copy(off, c).start()

    inner_x = unit(((lane > 0) | (ix > 0)) & ((lane < cols - 1) | (ix < nx - 1))).reshape(1, PTS, cols)
    z3 = lax.broadcasted_iota(jnp.int32, (planes, 1, cols), 0)
    inner_z = unit(((z3 > 0) | (iz > 0)) & ((z3 < planes - 1) | (iz < nz - 1)))
    for y in range(yel):
        w = inner_x
        if y == 0:
            w = w * unit((k_at > 0) | (iy > 0)).reshape(1, PTS, cols)
        if y == yel - 1:
            w = w * unit((k_at < ORDER) | (iy < ny - 1)).reshape(1, PTS, cols)
        keep[:, y * PTS:(y + 1) * PTS, :] = w * inner_z
    n_blk = PTS * PTS
    tile = (PTS, PTS, cols)
    kin, ens = [], []
    for e in range(layers):
        await_units(loads[e], in_sem.at[e])
        if e == 0:
            late_tabs = start(
                [(tx_hbm, tx_ref), (tyz_hbm, tyz_ref), (put_hbm, put_ref)], layers
            )
        at = pl.ds(e * PTS, PTS)
        mass = m[at].astype(jnp.float32)
        geo = [g[k, at].astype(jnp.float32) for k in range(6)]
        square = None
        for c in range(3):
            block = v[c, at]
            square = block * block if square is None else square + block * block
            pairs = [split(block[:, y * PTS:(y + 1) * PTS, :].reshape(n_blk, cols)) for y in range(yel)]
            whole = tuple(jnp.concatenate([p[s] for p in pairs], axis=0) for s in range(2))
            gr_all = along_x(whole, dx_ref[...])
            for y0 in range(0, yel, 2):
                r = dot(dyz_ref[...], stacked(pairs[y0:y0 + 2]))
                for s in range(2):
                    y = y0 + s
                    gr = gr_all[y * n_blk:(y + 1) * n_blk].reshape(tile)
                    gs = r[:n_blk, s * cols:(s + 1) * cols].reshape(tile)
                    gt = r[n_blk:, s * cols:(s + 1) * cols].reshape(tile)
                    g0, g1, g2, g3, g4, g5 = (t[:, y * PTS:(y + 1) * PTS, :] for t in geo)
                    fr = g0 * gr + g3 * gs + g4 * gt
                    fs = g3 * gr + g1 * gs + g5 * gt
                    ft = g4 * gr + g5 * gs + g2 * gt
                    ens.append(jnp.sum(gr * fr + gs * fs + gt * ft, axis=0))
                    flux[0, c, e, y] = fr
                    flux[1, c, e, y] = fs
                    flux[2, c, e, y] = ft
        kin.append(jnp.sum((mass * square).reshape(-1, PTS, cols), axis=0))
    mine = jnp.concatenate(
        [jnp.sum(tree(kin), 0, keepdims=True) * 0.5, jnp.sum(tree(ens), 0, keepdims=True)], axis=0
    )
    part[...] = mine

    kind = jnp.where(is_up, 1, 0)

    def scalar_copy(to):
        return pltpu.make_async_remote_copy(
            src_ref=part, dst_ref=parts.at[me], send_sem=ssend, recv_sem=srecv.at[kind],
            device_id=to, device_id_type=MESH,
        )

    def tell(t, ok):
        pl.when(ok)(lambda: scalar_copy(dev(t)).start())

    def meet():
        pl.semaphore_wait(barrier, heard)
        for_targets(lows, tell)

        @pl.when(is_up)
        def _():
            for_targets(ups, tell)

    across = (nx - 1) // 2 - ix // 2 + (nz - 1 - iz)
    ahead = across + jnp.where(is_low, half - 1 - iy, ny - 1 - iy)
    turn = jnp.where((ix % 2 == 1) & (ix < nx - 1), 1, 0) + jnp.where(iz < nz - 1, 1, 0)
    ahead = jnp.where(iy == half - 1, jnp.maximum(ahead, 1 + turn), ahead)
    early = ahead <= 1

    @pl.when(early)
    def _():
        meet()
    parts[me] = mine

    await_units(late_tabs, in_sem.at[layers])
    for e in range(layers):
        x = m[pl.ds(e * PTS, PTS)].astype(jnp.float32)
        put_field(3, e, [x[:, y * PTS:(y + 1) * PTS, :].reshape(n_blk, cols) for y in range(yel)])
    finish_channel(3)

    for c in range(3):
        for e in range(layers):
            fr, fs, ft = ([split(flux[k, c, e, y].reshape(n_blk, cols)) for y in range(yel)] for k in range(3))
            whole = tuple(jnp.concatenate([p[s] for p in fr], axis=0) for s in range(2))
            x = along_x(whole, tx_ref[...])
            blocks = [x[y * n_blk:(y + 1) * n_blk] for y in range(yel)]
            for y0 in range(0, yel, 4):
                r = dot(tyz_ref[0], quad(fs[y0:y0 + 4])) + dot(tyz_ref[1], quad(ft[y0:y0 + 4]))
                r = r[:2 * n_blk] + r[2 * n_blk:]
                for s in range(4):
                    deep = (s % 2) * n_blk
                    blocks[y0 + s] += r[deep:deep + n_blk, (s // 2) * cols:(s // 2 + 1) * cols]
            put_field(c, e, blocks)
        finish_channel(c)

    pack_sides()
    pl.when(jnp.logical_not(early))(meet)

    for off in OFFS:
        @pl.when(there(off))
        def _(off=off):
            copy_to(off).start()

    for c in range(4):
        send_faces(c)

    odd = ix % 2 == 1

    def relays():
        return [
            pltpu.make_async_remote_copy(
                src_ref=low, dst_ref=low, send_sem=ssend, recv_sem=lrecv,
                device_id={"gx": ix - k, "gy": iy + 1, "gz": iz}, device_id_type=MESH,
            )
            for k in range(2)
        ]

    def relay_on():
        for c in relays():
            c.start()

    def wait_rows(n, sem):
        rest = parts.at[pl.ds(0, n)]
        pltpu.make_async_copy(rest, rest, sem).wait()

    def low_sum():
        wait_rows(n_low - 1, srecv.at[0])
        low[...] = jnp.sum(parts[0:n_low], axis=0)

    def low_wait():
        pltpu.make_async_copy(low, low, lrecv).wait()

    @pl.when((iy == half - 1) & odd)
    def _():
        low_sum()
        relay_on()

    @pl.when(is_up & (iy < ny - 1) & odd)
    def _():
        low_wait()
        relay_on()

    def beside(i, n):
        return jnp.where(i > 0, 1, 0) + jnp.where(i < n - 1, 1, 0)

    bx, by, bz = (beside(i, n) for i, n in zip(here, sizes))
    edge = span(landing((1, 0, 1)))
    whole_x = span(landing((1, 0, 0)))
    corner = span(landing((0, 1, 1)))
    def await_neighbours(sem):
        for x, y, z in itertools.product(*(((0,), (1,), (1, 2))[min(n, 3) - 1] for n in sizes)):
            n = (
                x * (1 + y) * (whole_x + z * edge) + y * z * corner
                + y * span(ryface.at[0]) + z * span(rzface.at[0])
            )
            pl.when((bx == x) & (by == y) & (bz == z))(functools.partial(await_units, n, sem))

    await_neighbours(recv_sem)

    pshape = (4, total_rows)
    place = lax.broadcasted_iota(jnp.int32, (1, total_rows), 1)
    for s, dx in ((0, 1), (1, -1)):
        acc = jnp.zeros(pshape, jnp.float32)
        for off in XOFF:
            if off[0] != dx:
                continue
            x = rpack[XOFF.index(off)]
            hit = place >= 0
            shift = 0
            if off[1]:
                hit = hit & (place % rows == (0 if off[1] < 0 else rows - 1))
                shift += off[1] * (rows - 1)
            if off[2]:
                hit = hit & (place // rows == (0 if off[2] < 0 else planes - 1))
                shift += off[2] * (planes - 1) * rows
            if shift:
                x = pltpu.roll(x, shift % total_rows, 1)
            acc = acc + jnp.where(jnp.broadcast_to(hit & there(off), pshape), x, 0.0)
        hi, lo = split(acc)
        halo[s * 4:s * 4 + 4, :] = hi.astype(jnp.float32)
        halo[8 + s * 4:12 + s * 4, :] = lo.astype(jnp.float32)

    z1 = lax.broadcasted_iota(jnp.int32, (planes, cols), 0)

    def add_yz(c):
        for dy, y in ((-1, 0), (1, rows - 1)):
            acc = jnp.where(there((0, dy, 0)), ryface[YOFF.index((0, dy, 0)), c], 0.0)
            for dz, z in ((-1, 0), (1, planes - 1)):
                off = (0, dy, dz)
                acc = acc + jnp.where((z1 == z) & there(off), ryz[YZOFF.index(off), c], 0.0)
            field[c, :, y, :] = field[c, :, y, :] + acc
        for k, (dz, z) in enumerate(((-1, 0), (1, planes - 1))):
            field[c, z] = field[c, z] + jnp.where(there((0, 0, dz)), rzface[k, c], 0.0)

    for c in range(4):
        add_yz(c)
    halos = halo[...].astype(jnp.bfloat16)
    for e in range(layers):
        at = pl.ds(e * PTS, PTS)
        x = lax.dot_general(
            halos[:, e * n_rows:(e + 1) * n_rows], put_ref[...], (((0,), (0,)), ((), ())),
            preferred_element_type=jnp.float32,
        )
        w = keep[at]
        mass = (field[3, at] + x[:, 3 * cols:].reshape(PTS, rows, cols)) * w
        for c in range(3):
            a_out[c, at] = (field[c, at] + x[:, c * cols:(c + 1) * cols].reshape(PTS, rows, cols)) * w
            b_out[c, at] = mass * v[c, at]

    await_neighbours(send_sem)
    n_up = count - n_low

    sends_on = (iy >= half - 1) & (iy < ny - 1) & odd
    later = jnp.logical_not(sends_on)
    for low_one, relays_too in itertools.product((True, False), repeat=2):
        n = (n_low - 1 if low_one else count - 1) + (2 if relays_too else 0)
        ok = (is_low if low_one else is_up) & (sends_on if relays_too else later)
        pl.when(ok)(functools.partial(wait_rows, n, ssend))

    @pl.when(is_low & later)
    def _():
        low_sum()

    @pl.when(is_up & later)
    def _():
        low_wait()

    @pl.when(is_low)
    def _():
        wait_rows(n_up, srecv.at[1])

    @pl.when(is_up)
    def _():
        wait_rows(n_up - 1, srecv.at[1])

    total = jnp.sum(parts[n_low:count], axis=0) + low[...]
    total = jnp.sum(total, axis=1, keepdims=True)
    s_out[...] = jnp.broadcast_to(total, (2, cols))


def finish(a_ref, b_ref, s_ref, r_hbm, k_hbm, e_hbm, r, k, e, sem):
    chunks = r.shape[0]
    kin = s_ref[0:1, :]
    ens = s_ref[1:2, :]
    rayleigh = ens / (2.0 * kin)
    k[...] = kin[:, 0:1]
    e[...] = ens[:, 0:1]
    for c in range(chunks):
        r[c] = a_ref[c] - rayleigh[None] * b_ref[c]
        pltpu.make_async_copy(r.at[c], r_hbm.at[c], sem.at[0]).start()
    outs = [pltpu.make_async_copy(k, k_hbm, sem.at[1]), pltpu.make_async_copy(e, e_hbm, sem.at[2])]
    for c in outs:
        c.start()
    for c in outs:
        c.wait()
    pltpu.make_async_copy(r, r_hbm, sem.at[0]).wait()


def per_device(sizes, velocity, geometry, mass_weights):
    planes, rows, cols = mass_weights.shape
    f32 = jnp.float32
    count = sizes[0] * sizes[1] * sizes[2]
    vmem = pl.BlockSpec(memory_space=pltpu.VMEM)
    hbm = pl.BlockSpec(memory_space=pltpu.HBM)
    consts = tables(cols)
    layers = planes // PTS
    applied, weighted, scalars = pl.pallas_call(
        functools.partial(kernel, sizes),
        out_shape=(
            jax.ShapeDtypeStruct(velocity.shape, f32),
            jax.ShapeDtypeStruct(velocity.shape, f32),
            jax.ShapeDtypeStruct((2, cols), f32),
        ),
        in_specs=[hbm] * 8,
        out_specs=(vmem, vmem, vmem),
        scratch_shapes=[
            pltpu.VMEM(velocity.shape, f32),
            pltpu.VMEM(geometry.shape, geometry.dtype),
            pltpu.VMEM(mass_weights.shape, mass_weights.dtype),
            *[pltpu.VMEM(t.shape, t.dtype) for t in consts],
            pltpu.VMEM((3, 3, layers, rows // PTS, PTS, PTS, cols), f32),
            pltpu.VMEM((4, planes, rows, cols), f32),
            pltpu.VMEM((planes, rows, cols), f32),
            pltpu.VMEM((2, 4, planes * rows), f32),
            pltpu.VMEM((2, 4, planes, cols), f32),
            pltpu.VMEM((2, 2, 4, 1, cols), f32),
            pltpu.VMEM((len(XOFF), 4, planes * rows), f32),
            pltpu.VMEM((2, 4, planes, cols), f32),
            pltpu.VMEM((2, 4, rows, cols), f32),
            pltpu.VMEM((len(YZOFF), 4, 1, cols), f32),
            pltpu.VMEM((2, cols), f32),
            pltpu.VMEM((count + 2, 2, cols), f32),
            pltpu.VMEM((2, cols), f32),
            pltpu.VMEM((velocity.size * 8 // UNIT, 4, 128), f32),
            pltpu.VMEM((2, 4, rows, cols), f32),
            pltpu.VMEM(mass_weights.shape, f32),
            pltpu.VMEM((16, planes * rows), f32),
            pltpu.SemaphoreType.DMA((layers + 1,)),
            pltpu.SemaphoreType.DMA,
            pltpu.SemaphoreType.DMA,
            pltpu.SemaphoreType.DMA,
            pltpu.SemaphoreType.DMA((2,)),
            pltpu.SemaphoreType.DMA,
        ],
        compiler_params=pltpu.CompilerParams(
            collective_id=0, has_side_effects=True, vmem_limit_bytes=32 * 1024 * 1024
        ),
    )(*(pltpu.with_memory_space_constraint(t, pltpu.HBM) for t in (velocity, geometry, mass_weights, *consts)))
    one = jax.ShapeDtypeStruct((1, 1), f32)
    residual, kinetic, enstrophy = pl.pallas_call(
        finish,
        out_shape=(jax.ShapeDtypeStruct(velocity.shape, f32), one, one),
        in_specs=[vmem] * 3,
        out_specs=(hbm,) * 3,
        scratch_shapes=[
            pltpu.VMEM(velocity.shape, f32),
            pltpu.VMEM((1, 1), f32),
            pltpu.VMEM((1, 1), f32),
            pltpu.SemaphoreType.DMA((3,)),
        ],
        compiler_params=pltpu.CompilerParams(vmem_limit_bytes=8 * 1024 * 1024),
    )(applied, weighted, scalars)
    return residual, kinetic[0, 0], enstrophy[0, 0]


def solution(mesh):
    sizes = tuple(mesh.shape[a] for a in AXES)
    in_specs = (P(None, "gz", "gy", "gx"), P(None, "gz", "gy", "gx"), P("gz", "gy", "gx"))
    out_specs = (P(None, "gz", "gy", "gx"), P(), P())
    return jax.shard_map(
        functools.partial(per_device, sizes),
        mesh=mesh, in_specs=in_specs, out_specs=out_specs, check_vma=False,
    )
```

```python
import functools
import itertools
import math

import jax
import jax.numpy as jnp
import numpy as np
from jax import lax
from jax.experimental import pallas as pl
from jax.experimental.pallas import tpu as pltpu
from jax.sharding import PartitionSpec as P

ORDER = 7
PTS = ORDER + 1
UNIT = 4 * 128 * 4
MESH = pl.DeviceIdType.MESH
AXES = ("gx", "gy", "gz")
XOFF = [o for o in itertools.product((-1, 0, 1), repeat=3) if o[0] != 0]
YZOFF = [o for o in itertools.product((-1, 0, 1), repeat=3) if o[0] == 0 and o[1] != 0 and o[2] != 0]
YOFF = [(0, -1, 0), (0, 1, 0)]
FACES = YOFF + [(0, 0, -1), (0, 0, 1)]
OFFS = sorted(XOFF + YZOFF, key=lambda o: -sum(map(abs, o)))


def gll_derivative(poly_order):
    node_count = poly_order + 1
    abscissa = np.cos(np.pi * np.arange(node_count) / poly_order)
    legendre = np.zeros((node_count, node_count))
    for newton_step in range(60):
        legendre[:, 0] = 1.0
        legendre[:, 1] = abscissa
        for degree in range(2, node_count):
            legendre[:, degree] = (
                (2 * degree - 1) * abscissa * legendre[:, degree - 1]
                - (degree - 1) * legendre[:, degree - 2]
            ) / degree
        abscissa = abscissa - (abscissa * legendre[:, poly_order] - legendre[:, poly_order - 1]) / (
            node_count * legendre[:, poly_order]
        )
    abscissa = abscissa[::-1]
    end_values = legendre[::-1, poly_order]
    spacing = abscissa[:, None] - abscissa[None, :] + np.eye(node_count)
    deriv_table = end_values[:, None] / end_values[None, :] / spacing
    deriv_table = deriv_table * (1.0 - np.eye(node_count))
    deriv_table[0, 0] = -poly_order * node_count / 4.0
    deriv_table[poly_order, poly_order] = poly_order * node_count / 4.0
    return deriv_table.astype(np.float32)


def split_np(m):
    hi = m.astype(jnp.bfloat16)
    lo = (m - hi.astype(np.float32)).astype(jnp.bfloat16)
    return hi, lo


def tables(cols):
    d = gll_derivative(ORDER)
    eye = np.eye(PTS, dtype=np.float32)

    def lanes(mat):
        hi, lo = split_np(np.kron(np.eye(cols // PTS, dtype=np.float32), mat.T))
        return np.block([[hi, lo], [hi, np.zeros_like(lo)]])

    def paired(mat):
        hi, lo = split_np(mat)
        zero = np.zeros_like(hi)
        return np.concatenate([np.block([[t, t, zero, zero], [zero, zero, t, t]]) for t in (hi, lo)])

    hi, lo = split_np(np.concatenate([np.kron(eye, d), np.kron(d, eye)]))
    out = [lanes(d), np.concatenate([hi, hi, lo, lo], axis=1)]
    out.append(lanes(d.T))
    out.append(np.stack([paired(np.kron(eye, d.T)), paired(np.kron(d.T, eye))]))
    put = np.zeros((16, 4 * cols), np.float32)
    for c in range(4):
        for base in (0, 8):
            put[base + c, c * cols + cols - 1] = 1.0
            put[base + 4 + c, c * cols] = 1.0
    out.append(put.astype(jnp.bfloat16))
    return [jnp.asarray(t) for t in out]


def split(x):
    hi = x.astype(jnp.bfloat16)
    lo = (x - hi.astype(jnp.float32)).astype(jnp.bfloat16)
    return hi, lo


def dot(a, b):
    return jnp.dot(a, b, preferred_element_type=jnp.float32)


def along_x(pair, table):
    cols = table.shape[1] // 2
    r = dot(jnp.concatenate(pair, axis=1), table)
    return r[:, :cols] + r[:, cols:]


def tree(terms):
    while len(terms) > 1:
        odd = terms[len(terms) // 2 * 2:]
        terms = [a + b for a, b in zip(terms[::2], terms[1::2])] + odd
    return terms[0]


def quad(pairs):
    deep = [jnp.concatenate([*pairs[k], *pairs[k + 1]], axis=0) for k in (0, 2)]
    return jnp.concatenate(deep, axis=1)


def stacked(pairs):
    hi = jnp.concatenate([p[0] for p in pairs], axis=1)
    lo = jnp.concatenate([p[1] for p in pairs], axis=1)
    return jnp.concatenate([hi, lo, hi, lo], axis=0)


def kernel(
    sizes,
    v_hbm, g_hbm, m_hbm, dx_hbm, dyz_hbm, tx_hbm, tyz_hbm, put_hbm,
    a_out, b_out, s_out,
    v, g, m, dx_ref, dyz_ref, tx_ref, tyz_ref, put_ref, grad, field, ends, pack, yface, yzrow, rpack, ryface, rzface, ryz, part, parts, low, units, zface, keep, halo,
    in_sem, send_sem, recv_sem, ssend, srecv, lrecv,
):
    nx, ny, nz = sizes
    count = nx * ny * nz
    planes, rows, cols = v.shape[1:]
    layers = planes // PTS
    yel = rows // PTS
    ix, iy, iz = (lax.axis_index(a) for a in AXES)
    half = ny // 2
    n_low = half * nx * nz
    is_low = iy < half
    is_up = iy >= half

    def span(*refs):
        size = sum(math.prod(r.shape) * jnp.dtype(r.dtype).itemsize for r in refs)
        assert size % UNIT == 0
        return size // UNIT

    def await_units(n, sem):
        pltpu.make_async_copy(units.at[pl.ds(0, n)], units.at[pl.ds(0, n)], sem).wait()

    def start(pairs, k):
        for src, dst in pairs:
            pltpu.make_async_copy(src, dst, in_sem.at[k]).start()
        return span(*(dst for _, dst in pairs))

    def load_layer(e):
        at = pl.ds(e * PTS, PTS)
        return start(
            [(v_hbm.at[:, at], v.at[:, at]), (g_hbm.at[:, at], g.at[:, at])], e
        )

    mass_load = start([(m_hbm, m)], layers + 1)
    loads = [load_layer(0)]
    loads[0] += start([(dx_hbm, dx_ref), (dyz_hbm, dyz_ref)], 0)

    def rank(x, y, z):
        return (y * nx + x) * nz + z

    me = rank(ix, iy, iz)

    def for_targets(ys, act):
        if count > 64:
            def body(t):
                y, x, z = t // (nx * nz), lax.rem(t // nz, nx), lax.rem(t, nz)
                act((x, y, z), t != me)
            pl.loop(ys[0] * nx * nz, (ys[-1] + 1) * nx * nz)(body)
            return
        for y, x, z in itertools.product(ys, range(nx), range(nz)):
            act((x, y, z), rank(x, y, z) != me)

    lows, ups = range(half), range(half, ny)

    def dev(t):
        return dict(zip(AXES, t))

    barrier = pltpu.get_barrier_semaphore()

    def greet(t):
        pl.semaphore_signal(barrier, inc=1, device_id=dev(t), device_id_type=MESH)

    def greet_if(t, ok):
        pl.when(ok)(lambda: greet(t))

    def greet_low(t, ok):
        x, y, z = t
        near = (jnp.abs(ix - x) <= 1) & (jnp.abs(iz - z) <= 1) & (iy - y == 1)
        pl.when(near)(lambda: greet(t))

    for_targets(ups, greet_if)

    @pl.when(is_low)
    def _():
        for_targets(lows, greet_if)

    @pl.when(is_up)
    def _():
        for_targets(lows, greet_low)

    loads += [load_layer(e) for e in range(1, layers)]

    def cross(i, n):
        return 1 + jnp.where(i > 0, 1, 0) + jnp.where(i < n - 1, 1, 0)

    beyond = jnp.where(iy == half - 1, cross(ix, nx) * cross(iz, nz), 0)
    heard = jnp.where(is_low, n_low - 1 + beyond, count - 1)

    n_rows = PTS * rows
    four = (PTS, yel, PTS, cols)
    flat8 = (1, 1, PTS, cols)
    lane = lax.broadcasted_iota(jnp.int32, flat8, 3)
    k_at = lax.broadcasted_iota(jnp.int32, flat8, 2)

    def unit(mask):
        return jnp.where(mask, 1.0, 0.0).astype(jnp.float32)

    x_next = unit((lane % PTS == ORDER) & (lane < cols - 1))
    x_prev = unit((lane % PTS == 0) & (lane > 0))
    y_last = unit(k_at == ORDER)
    y_first = unit(k_at == 0)

    def assemble_xy(blocks):
        tiles = (PTS, PTS, cols)
        lane_joint = (x_next + x_prev).reshape(1, PTS, cols)
        at_last = jnp.broadcast_to((lane % PTS == ORDER).reshape(1, PTS, cols), tiles)
        last, first = y_last.reshape(1, PTS, cols), y_first.reshape(1, PTS, cols)
        xs = []
        for x in blocks:
            up = pltpu.roll(x, cols - 1, 1).reshape(tiles)
            down = pltpu.roll(x, 1, 1).reshape(tiles)
            xs.append(x.reshape(tiles) + jnp.where(at_last, up, down) * lane_joint)
        out = []
        for y in range(yel):
            t = xs[y]
            if y < yel - 1:
                t = t + pltpu.roll(xs[y + 1], PTS - 1, 1) * last
            if y > 0:
                t = t + pltpu.roll(xs[y - 1], 1, 1) * first
            out.append(t)
        return out

    def put_field(c, e, blocks):
        for y, t in enumerate(assemble_xy(blocks)):
            field[c, pl.ds(e * PTS, PTS), y * PTS:(y + 1) * PTS, :] = t

    pair_of = lax.broadcasted_iota(jnp.int32, (rows, cols), 1) // 2

    def pack_sides():
        step = cols // rows
        for k in range(planes // step):
            t = ends[pl.ds(k * step, step)].reshape(cols, cols).T
            for c in range(4):
                for s in range(2):
                    r = 2 * c + 1 - s
                    pack[s, c:c + 1, k * cols:(k + 1) * cols] = t[r:r + 1]

    def finish_channel(c):
        for e in range(1, layers):
            low = field[c, e * PTS - 1]
            high = field[c, e * PTS]
            both = low + high
            field[c, e * PTS - 1] = both
            field[c, e * PTS] = both
        for k in range(planes):
            t = pltpu.roll(field[c, k], 2 * c + 1, 1)
            ends[k] = jnp.where(pair_of == c, t, 0.0 if c == 3 else ends[k])
        for side, y in ((0, 0), (1, rows - 1)):
            face = field[c, :, y, :]
            yface[side, c] = face
            yzrow[side, 0, c] = face[0:1]
            yzrow[side, 1, c] = face[planes - 1:planes]
        zface[0, c] = field[c, 0]
        zface[1, c] = field[c, planes - 1]

    total_rows = planes * rows
    here = (ix, iy, iz)

    def there(off):
        ok = None
        for o, i, n in zip(off, here, sizes):
            if o:
                t = (i > 0) if o < 0 else (i < n - 1)
                ok = t if ok is None else ok & t
        return ok

    def side(o):
        return (o + 1) // 2

    def target(off):
        return {a: i + o for a, i, o in zip(AXES, here, off)}

    def part_of(dz):
        width = total_rows // layers // 2
        width = width if width % 128 == 0 else total_rows
        if dz == 0:
            return pl.ds(0, total_rows)
        return pl.ds(0 if dz < 0 else total_rows - width, width)

    def landing(off):
        if off[0]:
            return rpack.at[XOFF.index(off), :, part_of(-off[2])]
        return ryz.at[YZOFF.index(off)]

    def copy_to(off):
        opp = tuple(-o for o in off)
        if off[0]:
            src = pack.at[side(off[0]), :, part_of(off[2])]
        else:
            src = yzrow.at[side(off[1]), side(off[2])]
        return pltpu.make_async_remote_copy(
            src_ref=src, dst_ref=landing(opp), send_sem=send_sem, recv_sem=recv_sem,
            device_id=target(off), device_id_type=MESH,
        )

    def face_copy(off, c):
        k, opp = FACES.index(off), FACES.index(tuple(-o for o in off))
        src, dst = (yface, ryface) if off[1] else (zface, rzface)
        return pltpu.make_async_remote_copy(
            src_ref=src.at[k % 2, c], dst_ref=dst.at[opp % 2, c], send_sem=send_sem,
            recv_sem=recv_sem, device_id=target(off), device_id_type=MESH,
        )

    def send_faces(c):
        for off in FACES[::-1]:
            @pl.when(there(off))
            def _(off=off):
                face_copy(off, c).start()

    inner_x = unit(((lane > 0) | (ix > 0)) & ((lane < cols - 1) | (ix < nx - 1))).reshape(1, PTS, cols)
    z3 = lax.broadcasted_iota(jnp.int32, (planes, 1, cols), 0)
    inner_z = unit(((z3 > 0) | (iz > 0)) & ((z3 < planes - 1) | (iz < nz - 1)))
    for y in range(yel):
        w = inner_x
        if y == 0:
            w = w * unit((k_at > 0) | (iy > 0)).reshape(1, PTS, cols)
        if y == yel - 1:
            w = w * unit((k_at < ORDER) | (iy < ny - 1)).reshape(1, PTS, cols)
        keep[:, y * PTS:(y + 1) * PTS, :] = w * inner_z
    n_blk = PTS * PTS
    tile = (PTS, PTS, cols)
    await_units(mass_load, in_sem.at[layers + 1])
    for e in range(layers):
        x = m[pl.ds(e * PTS, PTS)].astype(jnp.float32)
        put_field(3, e, [x[:, y * PTS:(y + 1) * PTS, :].reshape(n_blk, cols) for y in range(yel)])
    finish_channel(3)

    kin, ens = [], []
    for e in range(layers):
        await_units(loads[e], in_sem.at[e])
        if e == 0:
            late_tabs = start(
                [(tx_hbm, tx_ref), (tyz_hbm, tyz_ref), (put_hbm, put_ref)], layers
            )
        at = pl.ds(e * PTS, PTS)
        mass = m[at].astype(jnp.float32)
        geo = [g[k, at].astype(jnp.float32) for k in range(3)]
        geo += [(g[k, at] + g[k, at]).astype(jnp.float32) for k in range(3, 6)]
        square = None
        for c in range(3):
            block = v[c, at]
            square = block * block if square is None else square + block * block
            pairs = [split(block[:, y * PTS:(y + 1) * PTS, :].reshape(n_blk, cols)) for y in range(yel)]
            whole = tuple(jnp.concatenate([p[s] for p in pairs], axis=0) for s in range(2))
            gr_all = along_x(whole, dx_ref[...])
            for y0 in range(0, yel, 2):
                r = dot(dyz_ref[...], stacked(pairs[y0:y0 + 2]))
                for s in range(2):
                    y = y0 + s
                    gr = gr_all[y * n_blk:(y + 1) * n_blk].reshape(tile)
                    gs = r[:n_blk, s * cols:(s + 1) * cols].reshape(tile)
                    gt = r[n_blk:, s * cols:(s + 1) * cols].reshape(tile)
                    g0, g1, g2, g33, g44, g55 = (t[:, y * PTS:(y + 1) * PTS, :] for t in geo)
                    form = gr * (g0 * gr + g33 * gs + g44 * gt) + gs * (g1 * gs + g55 * gt) + gt * (g2 * gt)
                    ens.append(jnp.sum(form, axis=0))
                    grad[0, c, e, y] = gr
                    grad[1, c, e, y] = gs
                    grad[2, c, e, y] = gt
        kin.append(jnp.sum((mass * square).reshape(-1, PTS, cols), axis=0))
    mine = jnp.concatenate(
        [jnp.sum(tree(kin), 0, keepdims=True) * 0.5, jnp.sum(tree(ens), 0, keepdims=True)], axis=0
    )
    part[...] = mine

    kind = jnp.where(is_up, 1, 0)

    def scalar_copy(to):
        return pltpu.make_async_remote_copy(
            src_ref=part, dst_ref=parts.at[me], send_sem=ssend, recv_sem=srecv.at[kind],
            device_id=to, device_id_type=MESH,
        )

    def tell(t, ok):
        pl.when(ok)(lambda: scalar_copy(dev(t)).start())

    def meet():
        pl.semaphore_wait(barrier, heard)
        for_targets(lows, tell)

        @pl.when(is_up)
        def _():
            for_targets(ups, tell)

    across = (nx - 1) // 2 - ix // 2 + (nz - 1 - iz)
    ahead = across + jnp.where(is_low, half - 1 - iy, ny - 1 - iy)
    turn = jnp.where((ix % 2 == 1) & (ix < nx - 1), 1, 0) + jnp.where(iz < nz - 1, 1, 0)
    ahead = jnp.where(iy == half - 1, jnp.maximum(ahead, 1 + turn), ahead)
    early = ahead <= 1

    @pl.when(early)
    def _():
        meet()
    parts[me] = mine

    await_units(late_tabs, in_sem.at[layers])

    metric = {
        (e, y): [g[k, pl.ds(e * PTS, PTS), pl.ds(y * PTS, PTS)].astype(jnp.float32) for k in range(6)]
        for e in range(layers) for y in range(yel)
    }

    def fluxes(c, e, y):
        g0, g1, g2, g3, g4, g5 = metric[e, y]
        gr, gs, gt = (grad[k, c, e, y] for k in range(3))
        return g0 * gr + g3 * gs + g4 * gt, g3 * gr + g1 * gs + g5 * gt, g4 * gr + g5 * gs + g2 * gt

    for c in range(3):
        for e in range(layers):
            fr, fs, ft = [], [], []
            for y in range(yel):
                for store, f in zip((fr, fs, ft), fluxes(c, e, y)):
                    store.append(split(f.reshape(n_blk, cols)))
            whole = tuple(jnp.concatenate([p[s] for p in fr], axis=0) for s in range(2))
            x = along_x(whole, tx_ref[...])
            blocks = [x[y * n_blk:(y + 1) * n_blk] for y in range(yel)]
            for y0 in range(0, yel, 4):
                r = dot(tyz_ref[0], quad(fs[y0:y0 + 4])) + dot(tyz_ref[1], quad(ft[y0:y0 + 4]))
                r = r[:2 * n_blk] + r[2 * n_blk:]
                for s in range(4):
                    deep = (s % 2) * n_blk
                    blocks[y0 + s] += r[deep:deep + n_blk, (s // 2) * cols:(s // 2 + 1) * cols]
            put_field(c, e, blocks)
        finish_channel(c)

    pack_sides()
    pl.when(jnp.logical_not(early))(meet)

    for off in OFFS:
        @pl.when(there(off))
        def _(off=off):
            copy_to(off).start()

    for c in range(4):
        send_faces(c)

    odd = ix % 2 == 1

    def relays():
        return [
            pltpu.make_async_remote_copy(
                src_ref=low, dst_ref=low, send_sem=ssend, recv_sem=lrecv,
                device_id={"gx": ix - k, "gy": iy + 1, "gz": iz}, device_id_type=MESH,
            )
            for k in range(2)
        ]

    def relay_on():
        for c in relays():
            c.start()

    def wait_rows(n, sem):
        rest = parts.at[pl.ds(0, n)]
        pltpu.make_async_copy(rest, rest, sem).wait()

    def low_sum():
        wait_rows(n_low - 1, srecv.at[0])
        low[...] = jnp.sum(parts[0:n_low], axis=0)

    def low_wait():
        pltpu.make_async_copy(low, low, lrecv).wait()

    @pl.when((iy == half - 1) & odd)
    def _():
        low_sum()
        relay_on()

    @pl.when(is_up & (iy < ny - 1) & odd)
    def _():
        low_wait()
        relay_on()

    def beside(i, n):
        return jnp.where(i > 0, 1, 0) + jnp.where(i < n - 1, 1, 0)

    bx, by, bz = (beside(i, n) for i, n in zip(here, sizes))
    edge = span(landing((1, 0, 1)))
    whole_x = span(landing((1, 0, 0)))
    corner = span(landing((0, 1, 1)))
    def await_neighbours(sem):
        for x, y, z in itertools.product(*(((0,), (1,), (1, 2))[min(n, 3) - 1] for n in sizes)):
            n = (
                x * (1 + y) * (whole_x + z * edge) + y * z * corner
                + y * span(ryface.at[0]) + z * span(rzface.at[0])
            )
            pl.when((bx == x) & (by == y) & (bz == z))(functools.partial(await_units, n, sem))

    await_neighbours(recv_sem)

    pshape = (4, total_rows)
    place = lax.broadcasted_iota(jnp.int32, (1, total_rows), 1)
    for s, dx in ((0, 1), (1, -1)):
        acc = jnp.zeros(pshape, jnp.float32)
        for off in XOFF:
            if off[0] != dx:
                continue
            x = rpack[XOFF.index(off)]
            hit = place >= 0
            shift = 0
            if off[1]:
                hit = hit & (place % rows == (0 if off[1] < 0 else rows - 1))
                shift += off[1] * (rows - 1)
            if off[2]:
                hit = hit & (place // rows == (0 if off[2] < 0 else planes - 1))
                shift += off[2] * (planes - 1) * rows
            if shift:
                x = pltpu.roll(x, shift % total_rows, 1)
            acc = acc + jnp.where(jnp.broadcast_to(hit & there(off), pshape), x, 0.0)
        hi, lo = split(acc)
        halo[s * 4:s * 4 + 4, :] = hi.astype(jnp.float32)
        halo[8 + s * 4:12 + s * 4, :] = lo.astype(jnp.float32)

    z1 = lax.broadcasted_iota(jnp.int32, (planes, cols), 0)

    def add_yz(c):
        for dy, y in ((-1, 0), (1, rows - 1)):
            acc = jnp.where(there((0, dy, 0)), ryface[YOFF.index((0, dy, 0)), c], 0.0)
            for dz, z in ((-1, 0), (1, planes - 1)):
                off = (0, dy, dz)
                acc = acc + jnp.where((z1 == z) & there(off), ryz[YZOFF.index(off), c], 0.0)
            field[c, :, y, :] = field[c, :, y, :] + acc
        for k, (dz, z) in enumerate(((-1, 0), (1, planes - 1))):
            field[c, z] = field[c, z] + jnp.where(there((0, 0, dz)), rzface[k, c], 0.0)

    for c in range(4):
        add_yz(c)
    halos = halo[...].astype(jnp.bfloat16)
    for e in range(layers):
        at = pl.ds(e * PTS, PTS)
        x = lax.dot_general(
            halos[:, e * n_rows:(e + 1) * n_rows], put_ref[...], (((0,), (0,)), ((), ())),
            preferred_element_type=jnp.float32,
        )
        w = keep[at]
        mass = (field[3, at] + x[:, 3 * cols:].reshape(PTS, rows, cols)) * w
        for c in range(3):
            a_out[c, at] = (field[c, at] + x[:, c * cols:(c + 1) * cols].reshape(PTS, rows, cols)) * w
            b_out[c, at] = mass * v[c, at]

    await_neighbours(send_sem)
    n_up = count - n_low

    sends_on = (iy >= half - 1) & (iy < ny - 1) & odd
    later = jnp.logical_not(sends_on)
    for low_one, relays_too in itertools.product((True, False), repeat=2):
        n = (n_low - 1 if low_one else count - 1) + (2 if relays_too else 0)
        ok = (is_low if low_one else is_up) & (sends_on if relays_too else later)
        pl.when(ok)(functools.partial(wait_rows, n, ssend))

    @pl.when(is_low & later)
    def _():
        low_sum()

    @pl.when(is_up & later)
    def _():
        low_wait()

    @pl.when(is_low)
    def _():
        wait_rows(n_up, srecv.at[1])

    @pl.when(is_up)
    def _():
        wait_rows(n_up - 1, srecv.at[1])

    total = jnp.sum(parts[n_low:count], axis=0) + low[...]
    total = jnp.sum(total, axis=1, keepdims=True)
    s_out[...] = jnp.broadcast_to(total, (2, cols))


def finish(a_ref, b_ref, s_ref, r_hbm, k_hbm, e_hbm, r, k, e, sem):
    chunks = r.shape[0]
    kin = s_ref[0:1, :]
    ens = s_ref[1:2, :]
    rayleigh = ens / (2.0 * kin)
    k[...] = kin[:, 0:1]
    e[...] = ens[:, 0:1]
    for c in range(chunks):
        r[c] = a_ref[c] - rayleigh[None] * b_ref[c]
        pltpu.make_async_copy(r.at[c], r_hbm.at[c], sem.at[0]).start()
    outs = [pltpu.make_async_copy(k, k_hbm, sem.at[1]), pltpu.make_async_copy(e, e_hbm, sem.at[2])]
    for c in outs:
        c.start()
    for c in outs:
        c.wait()
    pltpu.make_async_copy(r, r_hbm, sem.at[0]).wait()


def per_device(sizes, velocity, geometry, mass_weights):
    planes, rows, cols = mass_weights.shape
    f32 = jnp.float32
    count = sizes[0] * sizes[1] * sizes[2]
    vmem = pl.BlockSpec(memory_space=pltpu.VMEM)
    hbm = pl.BlockSpec(memory_space=pltpu.HBM)
    consts = tables(cols)
    layers = planes // PTS
    applied, weighted, scalars = pl.pallas_call(
        functools.partial(kernel, sizes),
        out_shape=(
            jax.ShapeDtypeStruct(velocity.shape, f32),
            jax.ShapeDtypeStruct(velocity.shape, f32),
            jax.ShapeDtypeStruct((2, cols), f32),
        ),
        in_specs=[hbm] * 8,
        out_specs=(vmem, vmem, vmem),
        scratch_shapes=[
            pltpu.VMEM(velocity.shape, f32),
            pltpu.VMEM(geometry.shape, geometry.dtype),
            pltpu.VMEM(mass_weights.shape, mass_weights.dtype),
            *[pltpu.VMEM(t.shape, t.dtype) for t in consts],
            pltpu.VMEM((3, 3, layers, rows // PTS, PTS, PTS, cols), f32),
            pltpu.VMEM((4, planes, rows, cols), f32),
            pltpu.VMEM((planes, rows, cols), f32),
            pltpu.VMEM((2, 4, planes * rows), f32),
            pltpu.VMEM((2, 4, planes, cols), f32),
            pltpu.VMEM((2, 2, 4, 1, cols), f32),
            pltpu.VMEM((len(XOFF), 4, planes * rows), f32),
            pltpu.VMEM((2, 4, planes, cols), f32),
            pltpu.VMEM((2, 4, rows, cols), f32),
            pltpu.VMEM((len(YZOFF), 4, 1, cols), f32),
            pltpu.VMEM((2, cols), f32),
            pltpu.VMEM((count + 2, 2, cols), f32),
            pltpu.VMEM((2, cols), f32),
            pltpu.VMEM((velocity.size * 8 // UNIT, 4, 128), f32),
            pltpu.VMEM((2, 4, rows, cols), f32),
            pltpu.VMEM(mass_weights.shape, f32),
            pltpu.VMEM((16, planes * rows), f32),
            pltpu.SemaphoreType.DMA((layers + 2,)),
            pltpu.SemaphoreType.DMA,
            pltpu.SemaphoreType.DMA,
            pltpu.SemaphoreType.DMA,
            pltpu.SemaphoreType.DMA((2,)),
            pltpu.SemaphoreType.DMA,
        ],
        compiler_params=pltpu.CompilerParams(
            collective_id=0, has_side_effects=True, vmem_limit_bytes=32 * 1024 * 1024
        ),
    )(*(pltpu.with_memory_space_constraint(t, pltpu.HBM) for t in (velocity, geometry, mass_weights, *consts)))
    one = jax.ShapeDtypeStruct((1, 1), f32)
    residual, kinetic, enstrophy = pl.pallas_call(
        finish,
        out_shape=(jax.ShapeDtypeStruct(velocity.shape, f32), one, one),
        in_specs=[vmem] * 3,
        out_specs=(hbm,) * 3,
        scratch_shapes=[
            pltpu.VMEM(velocity.shape, f32),
            pltpu.VMEM((1, 1), f32),
            pltpu.VMEM((1, 1), f32),
            pltpu.SemaphoreType.DMA((3,)),
        ],
        compiler_params=pltpu.CompilerParams(vmem_limit_bytes=8 * 1024 * 1024),
    )(applied, weighted, scalars)
    return residual, kinetic[0, 0], enstrophy[0, 0]


def solution(mesh):
    sizes = tuple(mesh.shape[a] for a in AXES)
    in_specs = (P(None, "gz", "gy", "gx"), P(None, "gz", "gy", "gx"), P("gz", "gy", "gx"))
    out_specs = (P(None, "gz", "gy", "gx"), P(), P())
    return jax.shard_map(
        functools.partial(per_device, sizes),
        mesh=mesh, in_specs=in_specs, out_specs=out_specs, check_vma=False,
    )
```

```python
import functools
import itertools
import math

import jax
import jax.numpy as jnp
import numpy as np
from jax import lax
from jax.experimental import pallas as pl
from jax.experimental.pallas import tpu as pltpu
from jax.sharding import PartitionSpec as P

ORDER = 7
PTS = ORDER + 1
UNIT = 4 * 128 * 4
MESH = pl.DeviceIdType.MESH
AXES = ("gx", "gy", "gz")
XOFF = [o for o in itertools.product((-1, 0, 1), repeat=3) if o[0] != 0]
YZOFF = [o for o in itertools.product((-1, 0, 1), repeat=3) if o[0] == 0 and o[1] != 0 and o[2] != 0]
YOFF = [(0, -1, 0), (0, 1, 0)]
FACES = YOFF + [(0, 0, -1), (0, 0, 1)]
OFFS = sorted(XOFF + YZOFF, key=lambda o: -sum(map(abs, o)))


def gll_derivative(poly_order):
    node_count = poly_order + 1
    abscissa = np.cos(np.pi * np.arange(node_count) / poly_order)
    legendre = np.zeros((node_count, node_count))
    for newton_step in range(60):
        legendre[:, 0] = 1.0
        legendre[:, 1] = abscissa
        for degree in range(2, node_count):
            legendre[:, degree] = (
                (2 * degree - 1) * abscissa * legendre[:, degree - 1]
                - (degree - 1) * legendre[:, degree - 2]
            ) / degree
        abscissa = abscissa - (abscissa * legendre[:, poly_order] - legendre[:, poly_order - 1]) / (
            node_count * legendre[:, poly_order]
        )
    abscissa = abscissa[::-1]
    end_values = legendre[::-1, poly_order]
    spacing = abscissa[:, None] - abscissa[None, :] + np.eye(node_count)
    deriv_table = end_values[:, None] / end_values[None, :] / spacing
    deriv_table = deriv_table * (1.0 - np.eye(node_count))
    deriv_table[0, 0] = -poly_order * node_count / 4.0
    deriv_table[poly_order, poly_order] = poly_order * node_count / 4.0
    return deriv_table.astype(np.float32)


def split_np(m):
    hi = m.astype(jnp.bfloat16)
    lo = (m - hi.astype(np.float32)).astype(jnp.bfloat16)
    return hi, lo


def tables(cols):
    d = gll_derivative(ORDER)
    eye = np.eye(PTS, dtype=np.float32)

    def lanes(mat):
        hi, lo = split_np(np.kron(np.eye(cols // PTS, dtype=np.float32), mat.T))
        return np.block([[hi, lo], [hi, np.zeros_like(lo)]])

    def paired(mat):
        hi, lo = split_np(mat)
        zero = np.zeros_like(hi)
        return np.concatenate([np.block([[t, t, zero, zero], [zero, zero, t, t]]) for t in (hi, lo)])

    hi, lo = split_np(np.concatenate([np.kron(eye, d), np.kron(d, eye)]))
    out = [lanes(d), np.concatenate([hi, hi, lo, lo], axis=1)]
    out.append(lanes(d.T))
    out.append(np.stack([paired(np.kron(eye, d.T)), paired(np.kron(d.T, eye))]))
    put = np.zeros((16, 4 * cols), np.float32)
    for c in range(4):
        for base in (0, 8):
            put[base + c, c * cols + cols - 1] = 1.0
            put[base + 4 + c, c * cols] = 1.0
    out.append(put.astype(jnp.bfloat16))
    return [jnp.asarray(t) for t in out]


def split(x):
    hi = x.astype(jnp.bfloat16)
    lo = (x - hi.astype(jnp.float32)).astype(jnp.bfloat16)
    return hi, lo


def dot(a, b):
    return jnp.dot(a, b, preferred_element_type=jnp.float32)


def along_x(pair, table):
    cols = table.shape[1] // 2
    r = dot(jnp.concatenate(pair, axis=1), table)
    return r[:, :cols] + r[:, cols:]


def tree(terms):
    while len(terms) > 1:
        odd = terms[len(terms) // 2 * 2:]
        terms = [a + b for a, b in zip(terms[::2], terms[1::2])] + odd
    return terms[0]


def quad(pairs):
    deep = [jnp.concatenate([*pairs[k], *pairs[k + 1]], axis=0) for k in (0, 2)]
    return jnp.concatenate(deep, axis=1)


def stacked(pairs):
    hi = jnp.concatenate([p[0] for p in pairs], axis=1)
    lo = jnp.concatenate([p[1] for p in pairs], axis=1)
    return jnp.concatenate([hi, lo, hi, lo], axis=0)


def kernel(
    sizes,
    v_hbm, g_hbm, m_hbm, dx_hbm, dyz_hbm, tx_hbm, tyz_hbm, put_hbm,
    a_out, b_out, s_out,
    v, g, m, dx_ref, dyz_ref, tx_ref, tyz_ref, put_ref, grad, field, ends, pack, yface, yzrow, rpack, ryface, rzface, ryz, part, parts, low, units, zface, keep, halo,
    in_sem, send_sem, recv_sem, ssend, srecv,
):
    nx, ny, nz = sizes
    count = nx * ny * nz
    planes, rows, cols = v.shape[1:]
    layers = planes // PTS
    yel = rows // PTS
    ix, iy, iz = (lax.axis_index(a) for a in AXES)
    half = ny // 2
    n_low = half * nx * nz
    is_low = iy < half
    is_up = iy >= half

    def span(*refs):
        size = sum(math.prod(r.shape) * jnp.dtype(r.dtype).itemsize for r in refs)
        assert size % UNIT == 0
        return size // UNIT

    def await_units(n, sem):
        pltpu.make_async_copy(units.at[pl.ds(0, n)], units.at[pl.ds(0, n)], sem).wait()

    def start(pairs, k):
        for src, dst in pairs:
            pltpu.make_async_copy(src, dst, in_sem.at[k]).start()
        return span(*(dst for _, dst in pairs))

    def load_layer(e):
        at = pl.ds(e * PTS, PTS)
        return start(
            [(v_hbm.at[:, at], v.at[:, at]), (g_hbm.at[:, at], g.at[:, at])], e
        )

    mass_load = start([(m_hbm, m)], layers)
    loads = [load_layer(0)]
    loads[0] += start([(dx_hbm, dx_ref), (dyz_hbm, dyz_ref)], 0)

    def rank(x, y, z):
        return (y * nx + x) * nz + z

    me = rank(ix, iy, iz)

    def for_targets(ys, act):
        if count > 64:
            def body(t):
                y, x, z = t // (nx * nz), lax.rem(t // nz, nx), lax.rem(t, nz)
                act((x, y, z), t != me)
            pl.loop(ys[0] * nx * nz, (ys[-1] + 1) * nx * nz)(body)
            return
        for y, x, z in itertools.product(ys, range(nx), range(nz)):
            act((x, y, z), rank(x, y, z) != me)

    lows, ups = range(half), range(half, ny)

    def dev(t):
        return dict(zip(AXES, t))

    barrier = pltpu.get_barrier_semaphore()

    def greet(t):
        pl.semaphore_signal(barrier, inc=1, device_id=dev(t), device_id_type=MESH)

    def greet_if(t, ok):
        pl.when(ok)(lambda: greet(t))

    def greet_low(t, ok):
        x, y, z = t
        near = (jnp.abs(ix - x) <= 1) & (jnp.abs(iz - z) <= 1) & (iy - y == 1)
        pl.when(near)(lambda: greet(t))

    for_targets(ups, greet_if)

    @pl.when(is_low)
    def _():
        for_targets(lows, greet_if)

    @pl.when(is_up)
    def _():
        for_targets(lows, greet_low)

    loads += [load_layer(e) for e in range(1, layers)]

    def cross(i, n):
        return 1 + jnp.where(i > 0, 1, 0) + jnp.where(i < n - 1, 1, 0)

    beyond = jnp.where(iy == half - 1, cross(ix, nx) * cross(iz, nz), 0)
    heard = jnp.where(is_low, n_low - 1 + beyond, count - 1)

    n_rows = PTS * rows
    four = (PTS, yel, PTS, cols)
    flat8 = (1, 1, PTS, cols)
    lane = lax.broadcasted_iota(jnp.int32, flat8, 3)
    k_at = lax.broadcasted_iota(jnp.int32, flat8, 2)

    def unit(mask):
        return jnp.where(mask, 1.0, 0.0).astype(jnp.float32)

    x_next = unit((lane % PTS == ORDER) & (lane < cols - 1))
    x_prev = unit((lane % PTS == 0) & (lane > 0))
    y_last = unit(k_at == ORDER)
    y_first = unit(k_at == 0)

    def assemble_xy(blocks):
        tiles = (PTS, PTS, cols)
        lane_joint = (x_next + x_prev).reshape(1, PTS, cols)
        at_last = jnp.broadcast_to((lane % PTS == ORDER).reshape(1, PTS, cols), tiles)
        last, first = y_last.reshape(1, PTS, cols), y_first.reshape(1, PTS, cols)
        xs = []
        for x in blocks:
            up = pltpu.roll(x, cols - 1, 1).reshape(tiles)
            down = pltpu.roll(x, 1, 1).reshape(tiles)
            xs.append(x.reshape(tiles) + jnp.where(at_last, up, down) * lane_joint)
        out = []
        for y in range(yel):
            t = xs[y]
            if y < yel - 1:
                t = t + pltpu.roll(xs[y + 1], PTS - 1, 1) * last
            if y > 0:
                t = t + pltpu.roll(xs[y - 1], 1, 1) * first
            out.append(t)
        return out

    def put_field(c, e, blocks):
        for y, t in enumerate(assemble_xy(blocks)):
            field[c, pl.ds(e * PTS, PTS), y * PTS:(y + 1) * PTS, :] = t

    pair_of = lax.broadcasted_iota(jnp.int32, (rows, cols), 1) // 2

    def pack_sides():
        step = cols // rows
        for k in range(planes // step):
            t = ends[pl.ds(k * step, step)].reshape(cols, cols).T
            for c in range(4):
                for s in range(2):
                    r = 2 * c + 1 - s
                    pack[s, c:c + 1, k * cols:(k + 1) * cols] = t[r:r + 1]

    def finish_channel(c):
        for e in range(1, layers):
            low = field[c, e * PTS - 1]
            high = field[c, e * PTS]
            both = low + high
            field[c, e * PTS - 1] = both
            field[c, e * PTS] = both
        for k in range(planes):
            t = pltpu.roll(field[c, k], 2 * c + 1, 1)
            ends[k] = jnp.where(pair_of == c, t, 0.0 if c == 3 else ends[k])
        for side, y in ((0, 0), (1, rows - 1)):
            face = field[c, :, y, :]
            yface[side, c] = face
            yzrow[side, 0, c] = face[0:1]
            yzrow[side, 1, c] = face[planes - 1:planes]
        zface[0, c] = field[c, 0]
        zface[1, c] = field[c, planes - 1]

    total_rows = planes * rows
    here = (ix, iy, iz)

    def there(off):
        ok = None
        for o, i, n in zip(off, here, sizes):
            if o:
                t = (i > 0) if o < 0 else (i < n - 1)
                ok = t if ok is None else ok & t
        return ok

    def side(o):
        return (o + 1) // 2

    def target(off):
        return {a: i + o for a, i, o in zip(AXES, here, off)}

    def part_of(dz):
        width = total_rows // layers // 2
        width = width if width % 128 == 0 else total_rows
        if dz == 0:
            return pl.ds(0, total_rows)
        return pl.ds(0 if dz < 0 else total_rows - width, width)

    def landing(off):
        if off[0]:
            return rpack.at[XOFF.index(off), :, part_of(-off[2])]
        return ryz.at[YZOFF.index(off)]

    def copy_to(off):
        opp = tuple(-o for o in off)
        if off[0]:
            src = pack.at[side(off[0]), :, part_of(off[2])]
        else:
            src = yzrow.at[side(off[1]), side(off[2])]
        return pltpu.make_async_remote_copy(
            src_ref=src, dst_ref=landing(opp), send_sem=send_sem, recv_sem=recv_sem,
            device_id=target(off), device_id_type=MESH,
        )

    def face_copy(off, c):
        k, opp = FACES.index(off), FACES.index(tuple(-o for o in off))
        src, dst = (yface, ryface) if off[1] else (zface, rzface)
        return pltpu.make_async_remote_copy(
            src_ref=src.at[k % 2, c], dst_ref=dst.at[opp % 2, c], send_sem=send_sem,
            recv_sem=recv_sem, device_id=target(off), device_id_type=MESH,
        )

    def send_faces(c):
        for off in FACES[::-1]:
            @pl.when(there(off))
            def _(off=off):
                face_copy(off, c).start()

    inner_x = unit(((lane > 0) | (ix > 0)) & ((lane < cols - 1) | (ix < nx - 1))).reshape(1, PTS, cols)
    z3 = lax.broadcasted_iota(jnp.int32, (planes, 1, cols), 0)
    inner_z = unit(((z3 > 0) | (iz > 0)) & ((z3 < planes - 1) | (iz < nz - 1)))
    for y in range(yel):
        w = inner_x
        if y == 0:
            w = w * unit((k_at > 0) | (iy > 0)).reshape(1, PTS, cols)
        if y == yel - 1:
            w = w * unit((k_at < ORDER) | (iy < ny - 1)).reshape(1, PTS, cols)
        keep[:, y * PTS:(y + 1) * PTS, :] = w * inner_z
    n_blk = PTS * PTS
    tile = (PTS, PTS, cols)
    across = (nx - 1) // 2 - ix // 2 + (nz - 1 - iz)
    ahead = across + jnp.where(is_low, half - 1 - iy, ny - 1 - iy)
    turn = jnp.where((ix % 2 == 1) & (ix < nx - 1), 1, 0) + jnp.where(iz < nz - 1, 1, 0)
    ahead = jnp.where(iy == half - 1, jnp.maximum(ahead, 1 + turn), ahead)
    early = ahead <= 1
    last_to_start = early & is_up

    def assemble_mass():
        for e in range(layers):
            x = m[pl.ds(e * PTS, PTS)].astype(jnp.float32)
            put_field(3, e, [x[:, y * PTS:(y + 1) * PTS, :].reshape(n_blk, cols) for y in range(yel)])
        finish_channel(3)

    await_units(mass_load, in_sem.at[layers])
    pl.when(jnp.logical_not(last_to_start))(assemble_mass)

    kin, ens = [], []
    for e in range(layers):
        await_units(loads[e], in_sem.at[e])
        if e == 0:
            late_tabs = start(
                [(tx_hbm, tx_ref), (tyz_hbm, tyz_ref), (put_hbm, put_ref)], 0
            )
        at = pl.ds(e * PTS, PTS)
        mass = m[at].astype(jnp.float32)
        geo = [g[k, at].astype(jnp.float32) for k in range(3)]
        geo += [(g[k, at] + g[k, at]).astype(jnp.float32) for k in range(3, 6)]
        square = None
        for c in range(3):
            block = v[c, at]
            square = block * block if square is None else square + block * block
            pairs = [split(block[:, y * PTS:(y + 1) * PTS, :].reshape(n_blk, cols)) for y in range(yel)]
            whole = tuple(jnp.concatenate([p[s] for p in pairs], axis=0) for s in range(2))
            gr_all = along_x(whole, dx_ref[...])
            for y0 in range(0, yel, 2):
                r = dot(dyz_ref[...], stacked(pairs[y0:y0 + 2]))
                for s in range(2):
                    y = y0 + s
                    gr = gr_all[y * n_blk:(y + 1) * n_blk].reshape(tile)
                    gs = r[:n_blk, s * cols:(s + 1) * cols].reshape(tile)
                    gt = r[n_blk:, s * cols:(s + 1) * cols].reshape(tile)
                    g0, g1, g2, g33, g44, g55 = (t[:, y * PTS:(y + 1) * PTS, :] for t in geo)
                    form = gr * (g0 * gr + g33 * gs + g44 * gt) + gs * (g1 * gs + g55 * gt) + gt * (g2 * gt)
                    ens.append(jnp.sum(form, axis=0))
                    grad[0, c, e, y] = gr
                    grad[1, c, e, y] = gs
                    grad[2, c, e, y] = gt
        kin.append(jnp.sum((mass * square).reshape(-1, PTS, cols), axis=0))
    mine = jnp.concatenate(
        [jnp.sum(tree(kin), 0, keepdims=True) * 0.5, jnp.sum(tree(ens), 0, keepdims=True)], axis=0
    )
    part[...] = mine

    kind = jnp.where(is_up, 1, 0)

    def scalar_copy(to):
        return pltpu.make_async_remote_copy(
            src_ref=part, dst_ref=parts.at[me], send_sem=ssend, recv_sem=srecv.at[kind],
            device_id=to, device_id_type=MESH,
        )

    def tell(t, ok):
        pl.when(ok)(lambda: scalar_copy(dev(t)).start())

    def meet():
        pl.semaphore_wait(barrier, heard)
        for_targets(lows, tell)

        @pl.when(is_up)
        def _():
            for_targets(ups, tell)

    @pl.when(early)
    def _():
        meet()
    parts[me] = mine
    pl.when(last_to_start)(assemble_mass)

    await_units(late_tabs, in_sem.at[0])

    metric = {
        (e, y): [g[k, pl.ds(e * PTS, PTS), pl.ds(y * PTS, PTS)].astype(jnp.float32) for k in range(6)]
        for e in range(layers) for y in range(yel)
    }

    def fluxes(c, e, y):
        g0, g1, g2, g3, g4, g5 = metric[e, y]
        gr, gs, gt = (grad[k, c, e, y] for k in range(3))
        return g0 * gr + g3 * gs + g4 * gt, g3 * gr + g1 * gs + g5 * gt, g4 * gr + g5 * gs + g2 * gt

    for c in range(3):
        for e in range(layers):
            fr, fs, ft = [], [], []
            for y in range(yel):
                for store, f in zip((fr, fs, ft), fluxes(c, e, y)):
                    store.append(split(f.reshape(n_blk, cols)))
            whole = tuple(jnp.concatenate([p[s] for p in fr], axis=0) for s in range(2))
            x = along_x(whole, tx_ref[...])
            blocks = [x[y * n_blk:(y + 1) * n_blk] for y in range(yel)]
            for y0 in range(0, yel, 4):
                r = dot(tyz_ref[0], quad(fs[y0:y0 + 4])) + dot(tyz_ref[1], quad(ft[y0:y0 + 4]))
                r = r[:2 * n_blk] + r[2 * n_blk:]
                for s in range(4):
                    deep = (s % 2) * n_blk
                    blocks[y0 + s] += r[deep:deep + n_blk, (s // 2) * cols:(s // 2 + 1) * cols]
            put_field(c, e, blocks)
        finish_channel(c)

    pack_sides()
    pl.when(jnp.logical_not(early))(meet)

    for off in OFFS:
        @pl.when(there(off))
        def _(off=off):
            copy_to(off).start()

    for c in range(4):
        send_faces(c)

    odd = ix % 2 == 1

    def relays():
        return [
            pltpu.make_async_remote_copy(
                src_ref=low, dst_ref=low, send_sem=ssend, recv_sem=srecv.at[0],
                device_id={"gx": ix - k, "gy": iy + 1, "gz": iz}, device_id_type=MESH,
            )
            for k in range(2)
        ]

    def relay_on():
        for c in relays():
            c.start()

    def wait_rows(n, sem):
        rest = parts.at[pl.ds(0, n)]
        pltpu.make_async_copy(rest, rest, sem).wait()

    def low_sum():
        wait_rows(n_low - 1, srecv.at[0])
        low[...] = jnp.sum(parts[0:n_low], axis=0)

    def low_wait():
        pltpu.make_async_copy(low, low, srecv.at[0]).wait()

    @pl.when((iy == half - 1) & odd)
    def _():
        low_sum()
        relay_on()

    @pl.when(is_up & (iy < ny - 1) & odd)
    def _():
        low_wait()
        relay_on()

    def beside(i, n):
        return jnp.where(i > 0, 1, 0) + jnp.where(i < n - 1, 1, 0)

    bx, by, bz = (beside(i, n) for i, n in zip(here, sizes))
    edge = span(landing((1, 0, 1)))
    whole_x = span(landing((1, 0, 0)))
    corner = span(landing((0, 1, 1)))
    def await_neighbours(sem):
        for x, y, z in itertools.product(*(((0,), (1,), (1, 2))[min(n, 3) - 1] for n in sizes)):
            n = (
                x * (1 + y) * (whole_x + z * edge) + y * z * corner
                + y * span(ryface.at[0]) + z * span(rzface.at[0])
            )
            pl.when((bx == x) & (by == y) & (bz == z))(functools.partial(await_units, n, sem))

    await_neighbours(recv_sem)

    pshape = (4, total_rows)
    place = lax.broadcasted_iota(jnp.int32, (1, total_rows), 1)
    for s, dx in ((0, 1), (1, -1)):
        acc = jnp.zeros(pshape, jnp.float32)
        for off in XOFF:
            if off[0] != dx:
                continue
            x = rpack[XOFF.index(off)]
            hit = place >= 0
            shift = 0
            if off[1]:
                hit = hit & (place % rows == (0 if off[1] < 0 else rows - 1))
                shift += off[1] * (rows - 1)
            if off[2]:
                hit = hit & (place // rows == (0 if off[2] < 0 else planes - 1))
                shift += off[2] * (planes - 1) * rows
            if shift:
                x = pltpu.roll(x, shift % total_rows, 1)
            acc = acc + jnp.where(jnp.broadcast_to(hit & there(off), pshape), x, 0.0)
        hi, lo = split(acc)
        halo[s * 4:s * 4 + 4, :] = hi.astype(jnp.float32)
        halo[8 + s * 4:12 + s * 4, :] = lo.astype(jnp.float32)

    z1 = lax.broadcasted_iota(jnp.int32, (planes, cols), 0)

    def add_yz(c):
        for dy, y in ((-1, 0), (1, rows - 1)):
            acc = jnp.where(there((0, dy, 0)), ryface[YOFF.index((0, dy, 0)), c], 0.0)
            for dz, z in ((-1, 0), (1, planes - 1)):
                off = (0, dy, dz)
                acc = acc + jnp.where((z1 == z) & there(off), ryz[YZOFF.index(off), c], 0.0)
            field[c, :, y, :] = field[c, :, y, :] + acc
        for k, (dz, z) in enumerate(((-1, 0), (1, planes - 1))):
            field[c, z] = field[c, z] + jnp.where(there((0, 0, dz)), rzface[k, c], 0.0)

    for c in range(4):
        add_yz(c)
    halos = halo[...].astype(jnp.bfloat16)
    for e in range(layers):
        at = pl.ds(e * PTS, PTS)
        x = lax.dot_general(
            halos[:, e * n_rows:(e + 1) * n_rows], put_ref[...], (((0,), (0,)), ((), ())),
            preferred_element_type=jnp.float32,
        )
        w = keep[at]
        mass = (field[3, at] + x[:, 3 * cols:].reshape(PTS, rows, cols)) * w
        for c in range(3):
            a_out[c, at] = (field[c, at] + x[:, c * cols:(c + 1) * cols].reshape(PTS, rows, cols)) * w
            b_out[c, at] = mass * v[c, at]

    await_neighbours(send_sem)
    n_up = count - n_low

    sends_on = (iy >= half - 1) & (iy < ny - 1) & odd
    later = jnp.logical_not(sends_on)
    for low_one, relays_too in itertools.product((True, False), repeat=2):
        n = (n_low - 1 if low_one else count - 1) + (2 if relays_too else 0)
        ok = (is_low if low_one else is_up) & (sends_on if relays_too else later)
        pl.when(ok)(functools.partial(wait_rows, n, ssend))

    @pl.when(is_low & later)
    def _():
        low_sum()

    @pl.when(is_up & later)
    def _():
        low_wait()

    @pl.when(is_low)
    def _():
        wait_rows(n_up, srecv.at[1])

    @pl.when(is_up)
    def _():
        wait_rows(n_up - 1, srecv.at[1])

    total = jnp.sum(parts[n_low:count], axis=0) + low[...]
    total = jnp.sum(total, axis=1, keepdims=True)
    s_out[...] = jnp.broadcast_to(total, (2, cols))


def finish(a_ref, b_ref, s_ref, r_hbm, k_hbm, e_hbm, r, k, e, sem):
    chunks = r.shape[0]
    kin = s_ref[0:1, :]
    ens = s_ref[1:2, :]
    rayleigh = ens / (2.0 * kin)
    k[...] = kin[:, 0:1]
    e[...] = ens[:, 0:1]
    for c in range(chunks):
        r[c] = a_ref[c] - rayleigh[None] * b_ref[c]
        pltpu.make_async_copy(r.at[c], r_hbm.at[c], sem.at[0]).start()
    outs = [pltpu.make_async_copy(k, k_hbm, sem.at[1]), pltpu.make_async_copy(e, e_hbm, sem.at[2])]
    for c in outs:
        c.start()
    for c in outs:
        c.wait()
    pltpu.make_async_copy(r, r_hbm, sem.at[0]).wait()


def per_device(sizes, velocity, geometry, mass_weights):
    planes, rows, cols = mass_weights.shape
    f32 = jnp.float32
    count = sizes[0] * sizes[1] * sizes[2]
    vmem = pl.BlockSpec(memory_space=pltpu.VMEM)
    hbm = pl.BlockSpec(memory_space=pltpu.HBM)
    consts = tables(cols)
    layers = planes // PTS
    applied, weighted, scalars = pl.pallas_call(
        functools.partial(kernel, sizes),
        out_shape=(
            jax.ShapeDtypeStruct(velocity.shape, f32),
            jax.ShapeDtypeStruct(velocity.shape, f32),
            jax.ShapeDtypeStruct((2, cols), f32),
        ),
        in_specs=[hbm] * 8,
        out_specs=(vmem, vmem, vmem),
        scratch_shapes=[
            pltpu.VMEM(velocity.shape, f32),
            pltpu.VMEM(geometry.shape, geometry.dtype),
            pltpu.VMEM(mass_weights.shape, mass_weights.dtype),
            *[pltpu.VMEM(t.shape, t.dtype) for t in consts],
            pltpu.VMEM((3, 3, layers, rows // PTS, PTS, PTS, cols), f32),
            pltpu.VMEM((4, planes, rows, cols), f32),
            pltpu.VMEM((planes, rows, cols), f32),
            pltpu.VMEM((2, 4, planes * rows), f32),
            pltpu.VMEM((2, 4, planes, cols), f32),
            pltpu.VMEM((2, 2, 4, 1, cols), f32),
            pltpu.VMEM((len(XOFF), 4, planes * rows), f32),
            pltpu.VMEM((2, 4, planes, cols), f32),
            pltpu.VMEM((2, 4, rows, cols), f32),
            pltpu.VMEM((len(YZOFF), 4, 1, cols), f32),
            pltpu.VMEM((2, cols), f32),
            pltpu.VMEM((count + 2, 2, cols), f32),
            pltpu.VMEM((2, cols), f32),
            pltpu.VMEM((velocity.size * 8 // UNIT, 4, 128), f32),
            pltpu.VMEM((2, 4, rows, cols), f32),
            pltpu.VMEM(mass_weights.shape, f32),
            pltpu.VMEM((16, planes * rows), f32),
            pltpu.SemaphoreType.DMA((layers + 1,)),
            pltpu.SemaphoreType.DMA,
            pltpu.SemaphoreType.DMA,
            pltpu.SemaphoreType.DMA,
            pltpu.SemaphoreType.DMA((2,)),
        ],
        compiler_params=pltpu.CompilerParams(
            collective_id=0, has_side_effects=True, vmem_limit_bytes=32 * 1024 * 1024
        ),
    )(*(pltpu.with_memory_space_constraint(t, pltpu.HBM) for t in (velocity, geometry, mass_weights, *consts)))
    one = jax.ShapeDtypeStruct((1, 1), f32)
    residual, kinetic, enstrophy = pl.pallas_call(
        finish,
        out_shape=(jax.ShapeDtypeStruct(velocity.shape, f32), one, one),
        in_specs=[vmem] * 3,
        out_specs=(hbm,) * 3,
        scratch_shapes=[
            pltpu.VMEM(velocity.shape, f32),
            pltpu.VMEM((1, 1), f32),
            pltpu.VMEM((1, 1), f32),
            pltpu.SemaphoreType.DMA((3,)),
        ],
        compiler_params=pltpu.CompilerParams(vmem_limit_bytes=8 * 1024 * 1024),
    )(applied, weighted, scalars)
    return residual, kinetic[0, 0], enstrophy[0, 0]


def solution(mesh):
    sizes = tuple(mesh.shape[a] for a in AXES)
    in_specs = (P(None, "gz", "gy", "gx"), P(None, "gz", "gy", "gx"), P("gz", "gy", "gx"))
    out_specs = (P(None, "gz", "gy", "gx"), P(), P())
    return jax.shard_map(
        functools.partial(per_device, sizes),
        mesh=mesh, in_specs=in_specs, out_specs=out_specs, check_vma=False,
    )
```

```python
import functools
import itertools
import math

import jax
import jax.numpy as jnp
import numpy as np
from jax import lax
from jax.experimental import pallas as pl
from jax.experimental.pallas import tpu as pltpu
from jax.sharding import PartitionSpec as P

ORDER = 7
PTS = ORDER + 1
UNIT = 4 * 128 * 4
MESH = pl.DeviceIdType.MESH
AXES = ("gx", "gy", "gz")
XOFF = [o for o in itertools.product((-1, 0, 1), repeat=3) if o[0] != 0]
YZOFF = [o for o in itertools.product((-1, 0, 1), repeat=3) if o[0] == 0 and o[1] != 0 and o[2] != 0]
YOFF = [(0, -1, 0), (0, 1, 0)]
FACES = YOFF + [(0, 0, -1), (0, 0, 1)]
OFFS = sorted(XOFF + YZOFF, key=lambda o: -sum(map(abs, o)))


def gll_derivative(poly_order):
    node_count = poly_order + 1
    abscissa = np.cos(np.pi * np.arange(node_count) / poly_order)
    legendre = np.zeros((node_count, node_count))
    for newton_step in range(60):
        legendre[:, 0] = 1.0
        legendre[:, 1] = abscissa
        for degree in range(2, node_count):
            legendre[:, degree] = (
                (2 * degree - 1) * abscissa * legendre[:, degree - 1]
                - (degree - 1) * legendre[:, degree - 2]
            ) / degree
        abscissa = abscissa - (abscissa * legendre[:, poly_order] - legendre[:, poly_order - 1]) / (
            node_count * legendre[:, poly_order]
        )
    abscissa = abscissa[::-1]
    end_values = legendre[::-1, poly_order]
    spacing = abscissa[:, None] - abscissa[None, :] + np.eye(node_count)
    deriv_table = end_values[:, None] / end_values[None, :] / spacing
    deriv_table = deriv_table * (1.0 - np.eye(node_count))
    deriv_table[0, 0] = -poly_order * node_count / 4.0
    deriv_table[poly_order, poly_order] = poly_order * node_count / 4.0
    return deriv_table.astype(np.float32)


def split_np(m):
    hi = m.astype(jnp.bfloat16)
    lo = (m - hi.astype(np.float32)).astype(jnp.bfloat16)
    return hi, lo


def tables(cols):
    d = gll_derivative(ORDER)
    eye = np.eye(PTS, dtype=np.float32)

    def lanes(mat):
        hi, lo = split_np(np.kron(np.eye(cols // PTS, dtype=np.float32), mat.T))
        return np.block([[hi, lo], [hi, np.zeros_like(lo)]])

    def paired(mat):
        hi, lo = split_np(mat)
        zero = np.zeros_like(hi)
        return np.concatenate([np.block([[t, t, zero, zero], [zero, zero, t, t]]) for t in (hi, lo)])

    hi, lo = split_np(np.concatenate([np.kron(eye, d), np.kron(d, eye)]))
    out = [lanes(d), np.concatenate([hi, hi, lo, lo], axis=1)]
    out.append(lanes(d.T))
    out.append(np.stack([paired(np.kron(eye, d.T)), paired(np.kron(d.T, eye))]))
    put = np.zeros((16, 4 * cols), np.float32)
    for c in range(4):
        for base in (0, 8):
            put[base + c, c * cols + cols - 1] = 1.0
            put[base + 4 + c, c * cols] = 1.0
    out.append(put.astype(jnp.bfloat16))
    return [jnp.asarray(t) for t in out]


def split(x):
    hi = x.astype(jnp.bfloat16)
    lo = (x - hi.astype(jnp.float32)).astype(jnp.bfloat16)
    return hi, lo


def dot(a, b):
    return jnp.dot(a, b, preferred_element_type=jnp.float32)


def along_x(pair, table):
    cols = table.shape[1] // 2
    r = dot(jnp.concatenate(pair, axis=1), table)
    return r[:, :cols] + r[:, cols:]


def tree(terms):
    while len(terms) > 1:
        odd = terms[len(terms) // 2 * 2:]
        terms = [a + b for a, b in zip(terms[::2], terms[1::2])] + odd
    return terms[0]


def quad(pairs):
    deep = [jnp.concatenate([*pairs[k], *pairs[k + 1]], axis=0) for k in (0, 2)]
    return jnp.concatenate(deep, axis=1)


def stacked(pairs):
    hi = jnp.concatenate([p[0] for p in pairs], axis=1)
    lo = jnp.concatenate([p[1] for p in pairs], axis=1)
    return jnp.concatenate([hi, lo, hi, lo], axis=0)


def kernel(
    sizes,
    v_hbm, g_hbm, m_hbm, dx_hbm, dyz_hbm, tx_hbm, tyz_hbm, put_hbm,
    a_out, b_out, s_out,
    v, g, m, dx_ref, dyz_ref, tx_ref, tyz_ref, put_ref, grad, field, ends, pack, yface, yzrow, rpack, ryface, rzface, ryz, part, parts, low, units, zface, keep, halo,
    in_sem, send_sem, recv_sem, ssend, srecv,
):
    nx, ny, nz = sizes
    count = nx * ny * nz
    planes, rows, cols = v.shape[1:]
    layers = planes // PTS
    yel = rows // PTS
    ix, iy, iz = (lax.axis_index(a) for a in AXES)
    half = ny // 2
    n_low = half * nx * nz
    is_low = iy < half
    is_up = iy >= half

    def span(*refs):
        size = sum(math.prod(r.shape) * jnp.dtype(r.dtype).itemsize for r in refs)
        assert size % UNIT == 0
        return size // UNIT

    def await_units(n, sem):
        pltpu.make_async_copy(units.at[pl.ds(0, n)], units.at[pl.ds(0, n)], sem).wait()

    def start(pairs, k):
        for src, dst in pairs:
            pltpu.make_async_copy(src, dst, in_sem.at[k]).start()
        return span(*(dst for _, dst in pairs))

    def load_layer(e):
        at = pl.ds(e * PTS, PTS)
        return start(
            [(v_hbm.at[:, at], v.at[:, at]), (g_hbm.at[:, at], g.at[:, at])], e
        )

    mass_load = start([(m_hbm, m)], layers)
    loads = [load_layer(0)]
    loads[0] += start([(dx_hbm, dx_ref), (dyz_hbm, dyz_ref)], 0)

    def rank(x, y, z):
        return (y * nx + x) * nz + z

    me = rank(ix, iy, iz)

    def for_targets(ys, act):
        if count > 64:
            def body(t):
                y, x, z = t // (nx * nz), lax.rem(t // nz, nx), lax.rem(t, nz)
                act((x, y, z), t != me)
            pl.loop(ys[0] * nx * nz, (ys[-1] + 1) * nx * nz)(body)
            return
        for y, x, z in itertools.product(ys, range(nx), range(nz)):
            act((x, y, z), rank(x, y, z) != me)

    lows, ups = range(half), range(half, ny)

    def dev(t):
        return dict(zip(AXES, t))

    barrier = pltpu.get_barrier_semaphore()

    def greet(t):
        pl.semaphore_signal(barrier, inc=1, device_id=dev(t), device_id_type=MESH)

    def greet_if(t, ok):
        pl.when(ok)(lambda: greet(t))

    def greet_low(t, ok):
        x, y, z = t
        near = (jnp.abs(ix - x) <= 1) & (jnp.abs(iz - z) <= 1) & (iy - y == 1)
        pl.when(near)(lambda: greet(t))

    for_targets(ups, greet_if)

    @pl.when(is_low)
    def _():
        for_targets(lows, greet_if)

    @pl.when(is_up)
    def _():
        for_targets(lows, greet_low)

    loads += [load_layer(e) for e in range(1, layers)]

    def cross(i, n):
        return 1 + jnp.where(i > 0, 1, 0) + jnp.where(i < n - 1, 1, 0)

    beyond = jnp.where(iy == half - 1, cross(ix, nx) * cross(iz, nz), 0)
    heard = jnp.where(is_low, n_low - 1 + beyond, count - 1)

    n_rows = PTS * rows
    four = (PTS, yel, PTS, cols)
    flat8 = (1, 1, PTS, cols)
    lane = lax.broadcasted_iota(jnp.int32, flat8, 3)
    k_at = lax.broadcasted_iota(jnp.int32, flat8, 2)

    def unit(mask):
        return jnp.where(mask, 1.0, 0.0).astype(jnp.float32)

    x_next = unit((lane % PTS == ORDER) & (lane < cols - 1))
    x_prev = unit((lane % PTS == 0) & (lane > 0))
    y_last = unit(k_at == ORDER)
    y_first = unit(k_at == 0)

    def assemble_xy(blocks):
        tiles = (PTS, PTS, cols)
        lane_joint = (x_next + x_prev).reshape(1, PTS, cols)
        at_last = jnp.broadcast_to((lane % PTS == ORDER).reshape(1, PTS, cols), tiles)
        last, first = y_last.reshape(1, PTS, cols), y_first.reshape(1, PTS, cols)
        joint = first + last
        in_last = jnp.broadcast_to((k_at == ORDER).reshape(1, PTS, cols), tiles)
        xs = []
        for x in blocks:
            up = pltpu.roll(x, cols - 1, 1).reshape(tiles)
            down = pltpu.roll(x, 1, 1).reshape(tiles)
            xs.append(x.reshape(tiles) + jnp.where(at_last, up, down) * lane_joint)
        out = []
        for y in range(yel):
            t = xs[y]
            after = pltpu.roll(xs[y + 1], PTS - 1, 1) if y < yel - 1 else None
            before = pltpu.roll(xs[y - 1], 1, 1) if y > 0 else None
            if before is None or after is None:
                t = t + (before * first if after is None else after * last)
            else:
                t = t + jnp.where(in_last, after, before) * joint
            out.append(t)
        return out

    def put_field(c, e, blocks):
        for y, t in enumerate(assemble_xy(blocks)):
            field[c, pl.ds(e * PTS, PTS), y * PTS:(y + 1) * PTS, :] = t

    pair_of = lax.broadcasted_iota(jnp.int32, (rows, cols), 1) // 2

    def pack_sides():
        step = cols // rows
        for k in range(planes // step):
            t = ends[pl.ds(k * step, step)].reshape(cols, cols).T
            for c in range(4):
                for s in range(2):
                    r = 2 * c + 1 - s
                    pack[s, c:c + 1, k * cols:(k + 1) * cols] = t[r:r + 1]

    def finish_channel(c):
        for e in range(1, layers):
            low = field[c, e * PTS - 1]
            high = field[c, e * PTS]
            both = low + high
            field[c, e * PTS - 1] = both
            field[c, e * PTS] = both
        for k in range(planes):
            t = pltpu.roll(field[c, k], 2 * c + 1, 1)
            ends[k] = jnp.where(pair_of == c, t, 0.0 if c == 3 else ends[k])
        for side, y in ((0, 0), (1, rows - 1)):
            face = field[c, :, y, :]
            yface[side, c] = face
            yzrow[side, 0, c] = face[0:1]
            yzrow[side, 1, c] = face[planes - 1:planes]
        zface[0, c] = field[c, 0]
        zface[1, c] = field[c, planes - 1]

    total_rows = planes * rows
    here = (ix, iy, iz)

    def there(off):
        ok = None
        for o, i, n in zip(off, here, sizes):
            if o:
                t = (i > 0) if o < 0 else (i < n - 1)
                ok = t if ok is None else ok & t
        return ok

    def side(o):
        return (o + 1) // 2

    def target(off):
        return {a: i + o for a, i, o in zip(AXES, here, off)}

    def part_of(dz):
        width = total_rows // layers // 2
        width = width if width % 128 == 0 else total_rows
        if dz == 0:
            return pl.ds(0, total_rows)
        return pl.ds(0 if dz < 0 else total_rows - width, width)

    def landing(off):
        if off[0]:
            return rpack.at[XOFF.index(off), :, part_of(-off[2])]
        return ryz.at[YZOFF.index(off)]

    def copy_to(off):
        opp = tuple(-o for o in off)
        if off[0]:
            src = pack.at[side(off[0]), :, part_of(off[2])]
        else:
            src = yzrow.at[side(off[1]), side(off[2])]
        return pltpu.make_async_remote_copy(
            src_ref=src, dst_ref=landing(opp), send_sem=send_sem, recv_sem=recv_sem,
            device_id=target(off), device_id_type=MESH,
        )

    def face_copy(off, c):
        k, opp = FACES.index(off), FACES.index(tuple(-o for o in off))
        src, dst = (yface, ryface) if off[1] else (zface, rzface)
        return pltpu.make_async_remote_copy(
            src_ref=src.at[k % 2, c], dst_ref=dst.at[opp % 2, c], send_sem=send_sem,
            recv_sem=recv_sem, device_id=target(off), device_id_type=MESH,
        )

    def send_faces(c):
        for off in FACES[::-1]:
            @pl.when(there(off))
            def _(off=off):
                face_copy(off, c).start()

    inner_x = unit(((lane > 0) | (ix > 0)) & ((lane < cols - 1) | (ix < nx - 1))).reshape(1, PTS, cols)
    z3 = lax.broadcasted_iota(jnp.int32, (planes, 1, cols), 0)
    inner_z = unit(((z3 > 0) | (iz > 0)) & ((z3 < planes - 1) | (iz < nz - 1)))
    for y in range(yel):
        w = inner_x
        if y == 0:
            w = w * unit((k_at > 0) | (iy > 0)).reshape(1, PTS, cols)
        if y == yel - 1:
            w = w * unit((k_at < ORDER) | (iy < ny - 1)).reshape(1, PTS, cols)
        keep[:, y * PTS:(y + 1) * PTS, :] = w * inner_z
    n_blk = PTS * PTS
    tile = (PTS, PTS, cols)
    across = (nx - 1) // 2 - ix // 2 + (nz - 1 - iz)
    ahead = across + jnp.where(is_low, half - 1 - iy, ny - 1 - iy)
    turn = jnp.where((ix % 2 == 1) & (ix < nx - 1), 1, 0) + jnp.where(iz < nz - 1, 1, 0)
    ahead = jnp.where(iy == half - 1, jnp.maximum(ahead, 1 + turn), ahead)
    early = ahead <= 1
    last_to_start = early & is_up

    def assemble_mass():
        for e in range(layers):
            x = m[pl.ds(e * PTS, PTS)].astype(jnp.float32)
            put_field(3, e, [x[:, y * PTS:(y + 1) * PTS, :].reshape(n_blk, cols) for y in range(yel)])
        finish_channel(3)

    await_units(mass_load, in_sem.at[layers])
    pl.when(jnp.logical_not(last_to_start))(assemble_mass)

    kin, ens = [], []
    for e in range(layers):
        await_units(loads[e], in_sem.at[e])
        if e == 0:
            late_tabs = start(
                [(tx_hbm, tx_ref), (tyz_hbm, tyz_ref), (put_hbm, put_ref)], 0
            )
        at = pl.ds(e * PTS, PTS)
        mass = m[at].astype(jnp.float32)
        geo = [g[k, at].astype(jnp.float32) for k in range(3)]
        geo += [(g[k, at] + g[k, at]).astype(jnp.float32) for k in range(3, 6)]
        square = None
        for c in range(3):
            block = v[c, at]
            square = block * block if square is None else square + block * block
            pairs = [split(block[:, y * PTS:(y + 1) * PTS, :].reshape(n_blk, cols)) for y in range(yel)]
            whole = tuple(jnp.concatenate([p[s] for p in pairs], axis=0) for s in range(2))
            gr_all = along_x(whole, dx_ref[...])
            for y0 in range(0, yel, 2):
                r = dot(dyz_ref[...], stacked(pairs[y0:y0 + 2]))
                for s in range(2):
                    y = y0 + s
                    gr = gr_all[y * n_blk:(y + 1) * n_blk].reshape(tile)
                    gs = r[:n_blk, s * cols:(s + 1) * cols].reshape(tile)
                    gt = r[n_blk:, s * cols:(s + 1) * cols].reshape(tile)
                    g0, g1, g2, g33, g44, g55 = (t[:, y * PTS:(y + 1) * PTS, :] for t in geo)
                    form = gr * (g0 * gr + g33 * gs + g44 * gt) + gs * (g1 * gs + g55 * gt) + gt * (g2 * gt)
                    ens.append(jnp.sum(form, axis=0))
                    grad[0, c, e, y] = gr
                    grad[1, c, e, y] = gs
                    grad[2, c, e, y] = gt
        kin.append(jnp.sum((mass * square).reshape(-1, PTS, cols), axis=0))
    mine = jnp.concatenate(
        [jnp.sum(tree(kin), 0, keepdims=True) * 0.5, jnp.sum(tree(ens), 0, keepdims=True)], axis=0
    )
    part[...] = mine

    kind = jnp.where(is_up, 1, 0)

    def scalar_copy(to):
        return pltpu.make_async_remote_copy(
            src_ref=part, dst_ref=parts.at[me], send_sem=ssend, recv_sem=srecv.at[kind],
            device_id=to, device_id_type=MESH,
        )

    def tell(t, ok):
        pl.when(ok)(lambda: scalar_copy(dev(t)).start())

    def meet():
        pl.semaphore_wait(barrier, heard)
        for_targets(lows, tell)

        @pl.when(is_up)
        def _():
            for_targets(ups, tell)

    @pl.when(early)
    def _():
        meet()
    parts[me] = mine
    pl.when(last_to_start)(assemble_mass)

    await_units(late_tabs, in_sem.at[0])

    metric = {
        (e, y): [g[k, pl.ds(e * PTS, PTS), pl.ds(y * PTS, PTS)].astype(jnp.float32) for k in range(6)]
        for e in range(layers) for y in range(yel)
    }

    def fluxes(c, e, y):
        g0, g1, g2, g3, g4, g5 = metric[e, y]
        gr, gs, gt = (grad[k, c, e, y] for k in range(3))
        return g0 * gr + g3 * gs + g4 * gt, g3 * gr + g1 * gs + g5 * gt, g4 * gr + g5 * gs + g2 * gt

    for c in range(3):
        for e in range(layers):
            fr, fs, ft = [], [], []
            for y in range(yel):
                for store, f in zip((fr, fs, ft), fluxes(c, e, y)):
                    store.append(split(f.reshape(n_blk, cols)))
            whole = tuple(jnp.concatenate([p[s] for p in fr], axis=0) for s in range(2))
            x = along_x(whole, tx_ref[...])
            blocks = [x[y * n_blk:(y + 1) * n_blk] for y in range(yel)]
            for y0 in range(0, yel, 4):
                r = dot(tyz_ref[0], quad(fs[y0:y0 + 4])) + dot(tyz_ref[1], quad(ft[y0:y0 + 4]))
                r = r[:2 * n_blk] + r[2 * n_blk:]
                for s in range(4):
                    deep = (s % 2) * n_blk
                    blocks[y0 + s] += r[deep:deep + n_blk, (s // 2) * cols:(s // 2 + 1) * cols]
            put_field(c, e, blocks)
        finish_channel(c)

    pack_sides()
    pl.when(jnp.logical_not(early))(meet)

    for off in OFFS:
        @pl.when(there(off))
        def _(off=off):
            copy_to(off).start()

    for c in range(4):
        send_faces(c)

    odd = ix % 2 == 1

    def relays():
        return [
            pltpu.make_async_remote_copy(
                src_ref=low, dst_ref=low, send_sem=ssend, recv_sem=srecv.at[0],
                device_id={"gx": ix - k, "gy": iy + 1, "gz": iz}, device_id_type=MESH,
            )
            for k in range(2)
        ]

    def relay_on():
        for c in relays():
            c.start()

    def wait_rows(n, sem):
        rest = parts.at[pl.ds(0, n)]
        pltpu.make_async_copy(rest, rest, sem).wait()

    def low_sum():
        wait_rows(n_low - 1, srecv.at[0])
        low[...] = jnp.sum(parts[0:n_low], axis=0)

    def low_wait():
        pltpu.make_async_copy(low, low, srecv.at[0]).wait()

    @pl.when((iy == half - 1) & odd)
    def _():
        low_sum()
        relay_on()

    @pl.when(is_up & (iy < ny - 1) & odd)
    def _():
        low_wait()
        relay_on()

    def beside(i, n):
        return jnp.where(i > 0, 1, 0) + jnp.where(i < n - 1, 1, 0)

    bx, by, bz = (beside(i, n) for i, n in zip(here, sizes))
    edge = span(landing((1, 0, 1)))
    whole_x = span(landing((1, 0, 0)))
    corner = span(landing((0, 1, 1)))
    def await_neighbours(sem):
        for x, y, z in itertools.product(*(((0,), (1,), (1, 2))[min(n, 3) - 1] for n in sizes)):
            n = (
                x * (1 + y) * (whole_x + z * edge) + y * z * corner
                + y * span(ryface.at[0]) + z * span(rzface.at[0])
            )
            pl.when((bx == x) & (by == y) & (bz == z))(functools.partial(await_units, n, sem))

    await_neighbours(recv_sem)

    pshape = (4, total_rows)
    place = lax.broadcasted_iota(jnp.int32, (1, total_rows), 1)
    for s, dx in ((0, 1), (1, -1)):
        acc = jnp.zeros(pshape, jnp.float32)
        for off in XOFF:
            if off[0] != dx:
                continue
            x = rpack[XOFF.index(off)]
            hit = place >= 0
            shift = 0
            if off[1]:
                hit = hit & (place % rows == (0 if off[1] < 0 else rows - 1))
                shift += off[1] * (rows - 1)
            if off[2]:
                hit = hit & (place // rows == (0 if off[2] < 0 else planes - 1))
                shift += off[2] * (planes - 1) * rows
            if shift:
                x = pltpu.roll(x, shift % total_rows, 1)
            acc = acc + jnp.where(jnp.broadcast_to(hit & there(off), pshape), x, 0.0)
        hi, lo = split(acc)
        halo[s * 4:s * 4 + 4, :] = hi.astype(jnp.float32)
        halo[8 + s * 4:12 + s * 4, :] = lo.astype(jnp.float32)

    z1 = lax.broadcasted_iota(jnp.int32, (planes, cols), 0)

    def add_yz(c):
        for dy, y in ((-1, 0), (1, rows - 1)):
            acc = jnp.where(there((0, dy, 0)), ryface[YOFF.index((0, dy, 0)), c], 0.0)
            for dz, z in ((-1, 0), (1, planes - 1)):
                off = (0, dy, dz)
                acc = acc + jnp.where((z1 == z) & there(off), ryz[YZOFF.index(off), c], 0.0)
            field[c, :, y, :] = field[c, :, y, :] + acc
        for k, (dz, z) in enumerate(((-1, 0), (1, planes - 1))):
            field[c, z] = field[c, z] + jnp.where(there((0, 0, dz)), rzface[k, c], 0.0)

    for c in range(4):
        add_yz(c)
    halos = halo[...].astype(jnp.bfloat16)
    for e in range(layers):
        at = pl.ds(e * PTS, PTS)
        x = lax.dot_general(
            halos[:, e * n_rows:(e + 1) * n_rows], put_ref[...], (((0,), (0,)), ((), ())),
            preferred_element_type=jnp.float32,
        )
        w = keep[at]
        mass = (field[3, at] + x[:, 3 * cols:].reshape(PTS, rows, cols)) * w
        for c in range(3):
            a_out[c, at] = (field[c, at] + x[:, c * cols:(c + 1) * cols].reshape(PTS, rows, cols)) * w
            b_out[c, at] = mass * v[c, at]

    await_neighbours(send_sem)
    n_up = count - n_low

    sends_on = (iy >= half - 1) & (iy < ny - 1) & odd
    later = jnp.logical_not(sends_on)
    for low_one, relays_too in itertools.product((True, False), repeat=2):
        n = (n_low - 1 if low_one else count - 1) + (2 if relays_too else 0)
        ok = (is_low if low_one else is_up) & (sends_on if relays_too else later)
        pl.when(ok)(functools.partial(wait_rows, n, ssend))

    @pl.when(is_low & later)
    def _():
        low_sum()

    @pl.when(is_up & later)
    def _():
        low_wait()

    @pl.when(is_low)
    def _():
        wait_rows(n_up, srecv.at[1])

    @pl.when(is_up)
    def _():
        wait_rows(n_up - 1, srecv.at[1])

    total = jnp.sum(parts[n_low:count], axis=0) + low[...]
    total = jnp.sum(total, axis=1, keepdims=True)
    s_out[...] = jnp.broadcast_to(total, (2, cols))


def finish(a_ref, b_ref, s_ref, r_hbm, k_hbm, e_hbm, r, k, e, sem):
    chunks = r.shape[0]
    kin = s_ref[0:1, :]
    ens = s_ref[1:2, :]
    rayleigh = ens / (2.0 * kin)
    k[...] = kin[:, 0:1]
    e[...] = ens[:, 0:1]
    for c in range(chunks):
        r[c] = a_ref[c] - rayleigh[None] * b_ref[c]
        pltpu.make_async_copy(r.at[c], r_hbm.at[c], sem.at[0]).start()
    outs = [pltpu.make_async_copy(k, k_hbm, sem.at[1]), pltpu.make_async_copy(e, e_hbm, sem.at[2])]
    for c in outs:
        c.start()
    for c in outs:
        c.wait()
    pltpu.make_async_copy(r, r_hbm, sem.at[0]).wait()


def per_device(sizes, velocity, geometry, mass_weights):
    planes, rows, cols = mass_weights.shape
    f32 = jnp.float32
    count = sizes[0] * sizes[1] * sizes[2]
    vmem = pl.BlockSpec(memory_space=pltpu.VMEM)
    hbm = pl.BlockSpec(memory_space=pltpu.HBM)
    consts = tables(cols)
    layers = planes // PTS
    applied, weighted, scalars = pl.pallas_call(
        functools.partial(kernel, sizes),
        out_shape=(
            jax.ShapeDtypeStruct(velocity.shape, f32),
            jax.ShapeDtypeStruct(velocity.shape, f32),
            jax.ShapeDtypeStruct((2, cols), f32),
        ),
        in_specs=[hbm] * 8,
        out_specs=(vmem, vmem, vmem),
        scratch_shapes=[
            pltpu.VMEM(velocity.shape, f32),
            pltpu.VMEM(geometry.shape, geometry.dtype),
            pltpu.VMEM(mass_weights.shape, mass_weights.dtype),
            *[pltpu.VMEM(t.shape, t.dtype) for t in consts],
            pltpu.VMEM((3, 3, layers, rows // PTS, PTS, PTS, cols), f32),
            pltpu.VMEM((4, planes, rows, cols), f32),
            pltpu.VMEM((planes, rows, cols), f32),
            pltpu.VMEM((2, 4, planes * rows), f32),
            pltpu.VMEM((2, 4, planes, cols), f32),
            pltpu.VMEM((2, 2, 4, 1, cols), f32),
            pltpu.VMEM((len(XOFF), 4, planes * rows), f32),
            pltpu.VMEM((2, 4, planes, cols), f32),
            pltpu.VMEM((2, 4, rows, cols), f32),
            pltpu.VMEM((len(YZOFF), 4, 1, cols), f32),
            pltpu.VMEM((2, cols), f32),
            pltpu.VMEM((count + 2, 2, cols), f32),
            pltpu.VMEM((2, cols), f32),
            pltpu.VMEM((velocity.size * 8 // UNIT, 4, 128), f32),
            pltpu.VMEM((2, 4, rows, cols), f32),
            pltpu.VMEM(mass_weights.shape, f32),
            pltpu.VMEM((16, planes * rows), f32),
            pltpu.SemaphoreType.DMA((layers + 1,)),
            pltpu.SemaphoreType.DMA,
            pltpu.SemaphoreType.DMA,
            pltpu.SemaphoreType.DMA,
            pltpu.SemaphoreType.DMA((2,)),
        ],
        compiler_params=pltpu.CompilerParams(
            collective_id=0, has_side_effects=True, vmem_limit_bytes=32 * 1024 * 1024
        ),
    )(*(pltpu.with_memory_space_constraint(t, pltpu.HBM) for t in (velocity, geometry, mass_weights, *consts)))
    one = jax.ShapeDtypeStruct((1, 1), f32)
    residual, kinetic, enstrophy = pl.pallas_call(
        finish,
        out_shape=(jax.ShapeDtypeStruct(velocity.shape, f32), one, one),
        in_specs=[vmem] * 3,
        out_specs=(hbm,) * 3,
        scratch_shapes=[
            pltpu.VMEM(velocity.shape, f32),
            pltpu.VMEM((1, 1), f32),
            pltpu.VMEM((1, 1), f32),
            pltpu.SemaphoreType.DMA((3,)),
        ],
        compiler_params=pltpu.CompilerParams(vmem_limit_bytes=8 * 1024 * 1024),
    )(applied, weighted, scalars)
    return residual, kinetic[0, 0], enstrophy[0, 0]


def solution(mesh):
    sizes = tuple(mesh.shape[a] for a in AXES)
    in_specs = (P(None, "gz", "gy", "gx"), P(None, "gz", "gy", "gx"), P("gz", "gy", "gx"))
    out_specs = (P(None, "gz", "gy", "gx"), P(), P())
    return jax.shard_map(
        functools.partial(per_device, sizes),
        mesh=mesh, in_specs=in_specs, out_specs=out_specs, check_vma=False,
    )
```
